32 devices in a mesh: data: 4 (over z), stage: 8 (over y, x, core).
Axes of the slice: x: 2, y: 2, z: 4, core: 2. Of those that a mesh axis runs over, the one named last changes fastest.
Arguments:
- master_up: float32 [8, 512, 2048], P('stage')
- master_down: float32 [8, 2048, 512], P('stage')
- mom1_up: float32 [8, 512, 2048], P('stage')
- mom1_down: float32 [8, 2048, 512], P('stage')
- mom2_up: float32 [8, 512, 2048], P('stage')
- mom2_down: float32 [8, 2048, 512], P('stage')
- grad_up: float32 [4, 8, 512, 2048], P('data', 'stage')
- grad_down: float32 [4, 8, 2048, 512], P('data', 'stage')
- stage_acts: bfloat16 [8, 2048, 512], P('stage', 'data')
- loss_grad: bfloat16 [2048, 512], P('data')
- next_batch: bfloat16 [16, 2048, 512], P(None, 'data')
- learn_rate: float32 [], replicated
- max_norm: float32 [], replicated
Outputs:
- output 1: float32 [8, 512, 2048], P('stage')
- output 2: float32 [8, 2048, 512], P('stage')
- output 3: float32 [8, 512, 2048], P('stage')
- output 4: float32 [8, 2048, 512], P('stage')
- output 5: float32 [8, 512, 2048], P('stage')
- output 6: float32 [8, 2048, 512], P('stage')
- output 7: bfloat16 [8, 16, 2048, 512], P('stage', None, 'data')
All inputs are finite; a program needn't handle non-finite values.
Results may differ from the reference program's by a relative error of at most 0.012201.
Values are sent between devices in bfloat16 or wider.
A program may use at most 1 GiB of HBM per device.

```python
import jax
import jax.numpy as jnp
from jax import lax

STAGES = 8
REPLICAS = 4
D = 512
FF = 2048
TOKENS = 512
MICROBATCHES = 16
ADAM_STEP = 8

ROWS = REPLICAS * TOKENS
BETA1 = 0.9
BETA2 = 0.95
ADAM_EPS = 1e-8
WEIGHT_DECAY = 0.1
NORM_EPS = 1e-6
SQRT_TWO_PI = 0.7978845608028654
GELU_CUBIC = 0.044715


def tanh_part(pre_act):
    return jnp.tanh(SQRT_TWO_PI * (pre_act + GELU_CUBIC * pre_act * pre_act * pre_act))


def gelu_tanh(pre_act):
    return 0.5 * pre_act * (1.0 + tanh_part(pre_act))


def gelu_pair(pre_act):
    tanh_val = tanh_part(pre_act)
    act_value = 0.5 * pre_act * (1.0 + tanh_val)
    act_slope = 0.5 * (1.0 + tanh_val) + 0.5 * pre_act * (1.0 - tanh_val * tanh_val) * SQRT_TWO_PI * (1.0 + 3.0 * GELU_CUBIC * pre_act * pre_act)
    return act_value, act_slope


def stage_backward(stage_in, master_up, master_down, loss_grad):
    up_bf = master_up.astype(jnp.bfloat16)
    down_bf = master_down.astype(jnp.bfloat16)

    def back_body(grad_in, stage_xs):
        rows_in, up_p, down_p = stage_xs
        pre_act = jnp.dot(rows_in, up_p, preferred_element_type=jnp.float32)
        act_value, act_slope = gelu_pair(pre_act)
        hidden = act_value.astype(jnp.bfloat16)
        d_hidden = jnp.dot(grad_in, down_p.T, preferred_element_type=jnp.float32)
        d_pre = (d_hidden * act_slope).astype(jnp.bfloat16)
        d_rows = (grad_in.astype(jnp.float32) + jnp.dot(d_pre, up_p.T, preferred_element_type=jnp.float32)).astype(jnp.bfloat16)
        dw_up = jnp.dot(rows_in.T, d_pre, preferred_element_type=jnp.float32)
        dw_down = jnp.dot(hidden.T, grad_in, preferred_element_type=jnp.float32)
        return d_rows, (dw_up, dw_down)

    _, (dw_up, dw_down) = lax.scan(back_body, loss_grad, (stage_in, up_bf, down_bf), reverse=True)
    return dw_up, dw_down


def mean_grads(grad_up, grad_down, stage_in, master_up, master_down, loss_grad):
    dw_up, dw_down = stage_backward(stage_in, master_up, master_down, loss_grad)
    gbar_up = (jnp.sum(grad_up, axis=0) + dw_up) / REPLICAS
    gbar_down = (jnp.sum(grad_down, axis=0) + dw_down) / REPLICAS
    return gbar_up, gbar_down


def adamw_update(master, first_mom, second_mom, grad_avg, clip_scale, learn_rate):
    scaled = clip_scale * grad_avg
    new_first = BETA1 * first_mom + (1.0 - BETA1) * scaled
    new_second = BETA2 * second_mom + (1.0 - BETA2) * scaled * scaled
    first_hat = new_first / (1.0 - BETA1 ** ADAM_STEP)
    second_hat = new_second / (1.0 - BETA2 ** ADAM_STEP)
    new_master = master - learn_rate * (first_hat / (jnp.sqrt(second_hat) + ADAM_EPS) + WEIGHT_DECAY * master)
    return new_master, new_first, new_second


def setup_inputs(seed: int = 0) -> dict:
    base_key = jax.random.key(seed)
    key_list = jax.random.split(base_key, 16)
    std_up = D ** -0.5
    std_down = 1.5 * (FF * STAGES) ** -0.5
    master_up = jax.random.normal(key_list[0], (STAGES, D, FF), jnp.float32) * std_up
    master_down = jax.random.normal(key_list[1], (STAGES, FF, D), jnp.float32) * std_down
    stage_acts = jax.random.normal(key_list[2], (STAGES, ROWS, D), jnp.float32).astype(jnp.bfloat16)
    loss_grad = jax.random.normal(key_list[3], (ROWS, D), jnp.float32).astype(jnp.bfloat16)
    next_batch = jax.random.normal(key_list[4], (MICROBATCHES, ROWS, D), jnp.float32).astype(jnp.bfloat16)
    grad_up = jax.random.normal(key_list[5], (REPLICAS, STAGES, D, FF), jnp.float32) * (0.4 * (TOKENS / STAGES) ** 0.5)
    grad_down = jax.random.normal(key_list[6], (REPLICAS, STAGES, FF, D), jnp.float32) * (0.6 * TOKENS ** 0.5)
    gbar_up, gbar_down = mean_grads(grad_up, grad_down, stage_acts, master_up, master_down, loss_grad)
    grad_norm = jnp.sqrt(jnp.sum(gbar_up * gbar_up) + jnp.sum(gbar_down * gbar_down))
    norm_frac = jax.random.uniform(key_list[7], (), jnp.float32, 0.35, 0.65)
    max_norm = norm_frac * grad_norm
    rms_up = norm_frac * jnp.sqrt(jnp.mean(gbar_up * gbar_up))
    rms_down = norm_frac * jnp.sqrt(jnp.mean(gbar_down * gbar_down))
    mom1_up = jax.random.normal(key_list[8], (STAGES, D, FF), jnp.float32) * (0.1 * rms_up)
    mom1_down = jax.random.normal(key_list[9], (STAGES, FF, D), jnp.float32) * (0.1 * rms_down)
    mom2_up = jax.random.uniform(key_list[10], (STAGES, D, FF), jnp.float32, 0.05, 0.15) * (rms_up * rms_up)
    mom2_down = jax.random.uniform(key_list[11], (STAGES, FF, D), jnp.float32, 0.05, 0.15) * (rms_down * rms_down)
    learn_rate = jax.random.uniform(key_list[12], (), jnp.float32, 0.1, 0.3) * std_down
    return dict(master_up=master_up, master_down=master_down, mom1_up=mom1_up, mom1_down=mom1_down, mom2_up=mom2_up, mom2_down=mom2_down, grad_up=grad_up, grad_down=grad_down, stage_acts=stage_acts, loss_grad=loss_grad, next_batch=next_batch, learn_rate=learn_rate, max_norm=max_norm)


def reference(master_up, master_down, mom1_up, mom1_down, mom2_up, mom2_down, grad_up, grad_down, stage_acts, loss_grad, next_batch, learn_rate, max_norm):
    gbar_up, gbar_down = mean_grads(grad_up, grad_down, stage_acts, master_up, master_down, loss_grad)
    grad_norm = jnp.sqrt(jnp.sum(gbar_up * gbar_up) + jnp.sum(gbar_down * gbar_down))
    clip_scale = jnp.minimum(1.0, max_norm / (grad_norm + NORM_EPS))
    new_up, new_mom1_up, new_mom2_up = adamw_update(master_up, mom1_up, mom2_up, gbar_up, clip_scale, learn_rate)
    new_down, new_mom1_down, new_mom2_down = adamw_update(master_down, mom1_down, mom2_down, gbar_down, clip_scale, learn_rate)
    up_bf = new_up.astype(jnp.bfloat16)
    down_bf = new_down.astype(jnp.bfloat16)

    def fwd_body(rows_in, weights):
        up_p, down_p = weights
        pre_act = jnp.dot(rows_in, up_p, preferred_element_type=jnp.float32)
        hidden = gelu_tanh(pre_act).astype(jnp.bfloat16)
        rows_out = (rows_in.astype(jnp.float32) + jnp.dot(hidden, down_p, preferred_element_type=jnp.float32)).astype(jnp.bfloat16)
        return rows_out, rows_out

    flat_batch = next_batch.reshape(MICROBATCHES * ROWS, D)
    _, stage_outs = lax.scan(fwd_body, flat_batch, (up_bf, down_bf))
    stage_outputs = stage_outs.reshape(STAGES, MICROBATCHES, ROWS, D)
    return (new_up, new_down, new_mom1_up, new_mom1_down, new_mom2_up, new_mom2_down, stage_outputs)
```

```python
import functools

import jax
import jax.numpy as jnp
from jax import lax
from jax.experimental import pallas as pl
from jax.experimental.pallas import tpu as pltpu
from jax.sharding import PartitionSpec as P

BETA1 = 0.9
BETA2 = 0.95
ADAM_EPS = 1e-8
WEIGHT_DECAY = 0.1
NORM_EPS = 1e-6
ADAM_STEP = 8
SQRT_TWO_PI = 0.7978845608028654
GELU_CUBIC = 0.044715

MESH = pl.DeviceIdType.MESH
F32 = jnp.float32
BF16 = jnp.bfloat16


def tanh_part(pre_act):
    return jnp.tanh(SQRT_TWO_PI * (pre_act + GELU_CUBIC * pre_act * pre_act * pre_act))


def gelu_tanh(pre_act):
    return 0.5 * pre_act * (1.0 + tanh_part(pre_act))


def gelu_pair(pre_act):
    tanh_val = tanh_part(pre_act)
    act_value = 0.5 * pre_act * (1.0 + tanh_val)
    act_slope = 0.5 * (1.0 + tanh_val) + 0.5 * pre_act * (1.0 - tanh_val * tanh_val) * SQRT_TWO_PI * (1.0 + 3.0 * GELU_CUBIC * pre_act * pre_act)
    return act_value, act_slope


def mat(left, right):
    return jnp.dot(left, right, preferred_element_type=F32)


def mat_nt(left, right):
    return lax.dot_general(left, right, (((1,), (1,)), ((), ())), preferred_element_type=F32)


def adamw_update(master, first_mom, second_mom, grad_avg, clip_scale, learn_rate):
    scaled = clip_scale * grad_avg
    new_first = BETA1 * first_mom + (1.0 - BETA1) * scaled
    new_second = BETA2 * second_mom + (1.0 - BETA2) * scaled * scaled
    first_hat = new_first / (1.0 - BETA1 ** ADAM_STEP)
    second_hat = new_second / (1.0 - BETA2 ** ADAM_STEP)
    new_master = master - learn_rate * (first_hat / (jnp.sqrt(second_hat) + ADAM_EPS) + WEIGHT_DECAY * master)
    return new_master, new_first, new_second


class Cfg:
    def __init__(self, reps, stages, width, hidden, rows, micro):
        self.R, self.S, self.D, self.FF, self.T, self.M = reps, stages, width, hidden, rows, micro
        self.nblk = hidden // width
        self.hb = self.nblk // 2
        self.NB = 4
        self.BR = rows // self.NB
        self.CR = width // 8
        self.K = hidden // self.CR
        self.UR = rows // 2
        self.NU = micro * rows // self.UR
        self.NS = 8
        self.LAG_MID = 2
        self.LAG_END = 6


def mega(cfg, lr_ref, mn_ref, acts, mu, md, dy, gu, gd, m1u, m1d, m2u, m2d, nb,
         gbu, gbd, c_out, ys,
         own, rbuf, wbuf, xin, ybuf, gin, gout, muf, ubf, vbf, ht, dpre, slope, m2b, av, at, sq, cbuf, cvec,
         ld_sem, ldw_sem, ldg_sem, ldm_sem, g_recv, g_send, rs_recv, rs_send, c_recv, c_send, w_recv, w_send,
         gb_recv, gb_send, x_recv, y_send, y_out, ou_sem, od_sem, co_sem):
    R, S, D, FF, T, M = cfg.R, cfg.S, cfg.D, cfg.FF, cfg.T, cfg.M
    nblk, hb, NB, BR, CR, K, UR, NU, NS = cfg.nblk, cfg.hb, cfg.NB, cfg.BR, cfg.CR, cfg.K, cfg.UR, cfg.NU, cfg.NS
    r = lax.axis_index("data")
    s = lax.axis_index("stage")
    last = S - 1
    is_end = (r == 0) | (r == R - 1)
    is_mid = jnp.logical_not(is_end)
    low = r < R // 2

    def ru(c):
        return (c // hb) * FF + (c % hb) * D

    def rv(c):
        return ru(c) + FF // 2

    def ds(start, size):
        return pl.ds(pl.multiple_of(start, size), size)

    barrier = pltpu.get_barrier_semaphore()

    @pl.loop(0, R * S)
    def _(dev):
        pl.semaphore_signal(barrier, inc=1, device_id=(dev // S, dev % S), device_id_type=MESH)

    act_load = pltpu.make_async_copy(acts, av, ld_sem)
    act_load.start()
    w_loads = []
    for c in range(nblk):
        w_loads.append(pltpu.make_async_copy(mu.at[:, c * D:(c + 1) * D], muf.at[ru(c):ru(c) + D, :], ldw_sem.at[c]))
    for c in range(nblk):
        w_loads.append(pltpu.make_async_copy(md.at[c * D:(c + 1) * D, :], muf.at[rv(c):rv(c) + D, :], ldw_sem.at[nblk + c]))
    for load in w_loads:
        load.start()

    @pl.when(s == last)
    def _():
        for j in range(NB):
            pltpu.make_async_copy(dy.at[j * BR:(j + 1) * BR, :], gin.at[j * BR:(j + 1) * BR, :], g_recv.at[j]).start()

    g_loads = []
    for c in range(nblk):
        g_loads.append(pltpu.make_async_copy(gu.at[:, c * D:(c + 1) * D], own.at[ru(c):ru(c) + D, :], ldg_sem.at[c]))
        g_loads.append(pltpu.make_async_copy(gd.at[c * D:(c + 1) * D, :], own.at[rv(c):rv(c) + D, :], ldg_sem.at[nblk + c]))
    for load in g_loads:
        load.start()

    act_load.wait()
    at[...] = av[...].astype(F32).T.astype(BF16)
    for c in range(nblk):
        w_loads[c].wait()
        ubf[c * D:(c + 1) * D, :] = muf[ru(c):ru(c) + D, :].astype(BF16)

    @pl.loop(0, nblk * NB)
    def _(it):
        c, j = it // NB, it % NB
        pre = mat(av[ds(j * BR, BR), :], ubf[ds(c * D, D), :])
        act_value, act_slope = gelu_pair(pre)
        slope[ds(c * T + j * BR, BR), :] = act_slope
        ht[ds(c * D, D), ds(j * BR, BR)] = act_value.T.astype(BF16)

    for c in range(nblk):
        w_loads[nblk + c].wait()
        vbf[c * D:(c + 1) * D, :] = muf[rv(c):rv(c) + D, :].astype(BF16)

    pl.semaphore_wait(barrier, R * S)

    @pl.when(s == 0)
    def _():
        @pl.loop(0, NU)
        def _(u):
            pltpu.make_async_copy(nb.at[ds(u * UR, UR), :], xin.at[ds(u * UR, UR), :], x_recv.at[u]).start()

    def g_copy(j):
        rows = ds(j * BR, BR)
        return pltpu.make_async_remote_copy(gout.at[rows, :], gin.at[rows, :], g_send.at[j], g_recv.at[j],
                                            device_id={"stage": s - 1}, device_id_type=MESH)

    @pl.loop(0, NB)
    def _(j):
        rows = ds(j * BR, BR)
        pltpu.make_async_copy(gin.at[rows, :], gin.at[rows, :], g_recv.at[j]).wait()
        g = gin[rows, :]
        for c in range(nblk):
            part = ds(c * T + j * BR, BR)
            dpre[part, :] = (mat_nt(g, vbf[c * D:(c + 1) * D, :]) * slope[part, :]).astype(BF16)

        @pl.when(s > 0)
        def _():
            total = None
            for c in range(nblk):
                piece = mat_nt(dpre[ds(c * T + j * BR, BR), :], ubf[c * D:(c + 1) * D, :])
                total = piece if total is None else total + piece
            gout[rows, :] = (g.astype(F32) + total).astype(BF16)
            g_copy(j).start()

    for load in g_loads:
        load.wait()
    half_d = D // 2

    @pl.loop(0, nblk * 2)
    def _(it):
        c, m = it // 2, it % 2
        up_rows = ds(ru(c) + m * half_d, half_d)
        down_rows = ds(rv(c) + m * half_d, half_d)
        own[up_rows, :] += mat(at[ds(m * half_d, half_d), :], dpre[ds(c * T, T), :])
        own[down_rows, :] += mat(ht[ds(c * D + m * half_d, half_d), :], gin[...])

    def moment_loads(half):
        out = []
        for b in range(hb):
            cols = slice((half * hb + b) * D, (half * hb + b + 1) * D)
            out.append(pltpu.make_async_copy(m1u.at[:, cols], slope.at[b * D:(b + 1) * D, :], ldm_sem.at[b]))
            out.append(pltpu.make_async_copy(m2u.at[:, cols], m2b.at[b * D:(b + 1) * D, :], ldm_sem.at[hb + b]))
            out.append(pltpu.make_async_copy(m1d.at[cols, :], slope.at[FF // 2 + b * D:FF // 2 + (b + 1) * D, :], ldm_sem.at[2 * hb + b]))
            out.append(pltpu.make_async_copy(m2d.at[cols, :], m2b.at[FF // 2 + b * D:FF // 2 + (b + 1) * D, :], ldm_sem.at[3 * hb + b]))
        return out

    for half, where in ((0, r == 0), (1, r == R - 1)):
        @pl.when(where)
        def _():
            for load in moment_loads(half):
                load.start()

    def half_rows(half, k):
        return ds(half * FF + k * CR, CR)

    def await_f32(sem, half, k):
        rows = half_rows(half, k)
        pltpu.make_async_copy(own.at[rows, :], own.at[rows, :], sem.at[half, k]).wait()

    def rs_copy(src, half, k):
        rows = half_rows(half, k)
        return pltpu.make_async_remote_copy(src.at[rows, :], rbuf.at[rows, :], rs_send.at[half, k], rs_recv.at[half, k],
                                            device_id={"data": r + 2 * half - 1}, device_id_type=MESH)

    rs_near = jnp.where(low, 1, 0)
    rs_far = 1 - rs_near
    lag = jnp.where(is_end, cfg.LAG_END, cfg.LAG_MID)
    sq[...] = jnp.zeros_like(sq)

    @pl.loop(0, K + cfg.LAG_END)
    def _(i):
        @pl.when((i < K) & is_end)
        def _():
            rs_copy(own, rs_near, i).start()

        @pl.when((i < K) & is_mid)
        def _():
            await_f32(rs_recv, rs_near, i)
            rows = half_rows(rs_near, i)
            rbuf[rows, :] += own[rows, :]
            rs_copy(rbuf, rs_near, i).start()

        k = i - lag

        @pl.when((k >= 0) & (k < K) & is_mid)
        def _():
            await_f32(rs_recv, rs_far, k)
            rows = half_rows(rs_far, k)
            rbuf[rows, :] += own[rows, :]
            rs_copy(rbuf, rs_far, k).start()

        @pl.when((k >= 0) & (k < K) & is_end)
        def _():
            await_f32(rs_recv, rs_far, k)
            rows = half_rows(rs_far, k)
            mean = (own[rows, :] + rbuf[rows, :]) * (1.0 / R)
            own[rows, :] = mean
            sq[...] += jnp.sum((mean * mean).reshape(CR // 8, 8, D), axis=0)

    mine = jnp.where(r == 0, s, S + s)
    me = r * S + s

    def c_copy(dev):
        return pltpu.make_async_remote_copy(cbuf.at[mine], cbuf.at[mine], c_send.at[dev], c_recv.at[mine],
                                            device_id=(dev // S, dev % S), device_id_type=MESH)

    @pl.when(is_end)
    def _():
        part = sq[:, 0:128]
        for q in range(1, D // 128):
            part = part + sq[:, q * 128:(q + 1) * 128]
        cbuf[mine] = part

        @pl.loop(0, K)
        def _(k):
            rs_copy(own, rs_near, k).wait_send()

        @pl.loop(0, R * S)
        def _(dev):
            @pl.when(dev != me)
            def _():
                c_copy(dev).start()

    @pl.loop(0, 2 * S)
    def _(slot):
        @pl.when(is_mid | (slot != mine))
        def _():
            pltpu.make_async_copy(cbuf.at[slot], cbuf.at[slot], c_recv.at[slot]).wait()

    total_sq = cbuf[0]
    for slot in range(1, 2 * S):
        total_sq = total_sq + cbuf[slot]
    total_sq = jnp.sum(jnp.sum(total_sq, axis=0, keepdims=True), axis=1, keepdims=True)
    grad_norm = jnp.sqrt(jnp.broadcast_to(total_sq, (8, 128)))
    cvec[...] = jnp.minimum(1.0, mn_ref[0] / (grad_norm + NORM_EPS))
    pltpu.make_async_copy(cvec, c_out, co_sem).start()

    for half, where in ((0, r == 0), (1, r == R - 1)):
        @pl.when(where)
        def _():
            for load in moment_loads(half):
                load.wait()

    ag_near = 1 - rs_near
    ag_far = rs_near

    def w_copy(half, k):
        rows = half_rows(half, k)
        return pltpu.make_async_remote_copy(wbuf.at[rows, :], wbuf.at[rows, :], w_send.at[half, k], w_recv.at[half, k],
                                            device_id={"data": r + 1 - 2 * half}, device_id_type=MESH)

    def await_w(half, k):
        rows = half_rows(half, k)
        pltpu.make_async_copy(wbuf.at[rows, :], wbuf.at[rows, :], w_recv.at[half, k]).wait()

    @pl.loop(0, K + cfg.LAG_MID)
    def _(i):
        @pl.when((i < K) & is_end)
        def _():
            rows = half_rows(ag_near, i)
            local = ds(i * CR, CR)
            clip = cvec[0:1, 0:1]
            new_master, _, _ = adamw_update(muf[rows, :], slope[local, :], m2b[local, :], own[rows, :], clip, lr_ref[0])
            wbuf[rows, :] = new_master.astype(BF16)
            w_copy(ag_near, i).start()

        @pl.when((i < K) & is_mid)
        def _():
            await_w(ag_near, i)
            w_copy(ag_near, i).start()

        k = i - cfg.LAG_MID

        @pl.when((k >= 0) & is_mid)
        def _():
            await_w(ag_far, k)
            w_copy(ag_far, k).start()

    @pl.when(is_end)
    def _():
        @pl.loop(0, K)
        def _(k):
            await_w(ag_far, k)

    def gb_copy(half, k):
        rows = half_rows(half, k)
        return pltpu.make_async_remote_copy(own.at[rows, :], own.at[rows, :], gb_send.at[half, k], gb_recv.at[half, k],
                                            device_id={"data": r + 1 - 2 * half}, device_id_type=MESH)

    def gb_store(half, k):
        rows = half_rows(half, k)

        @pl.when(k < K // 2)
        def _():
            flat = k * CR
            cols = ds((half * hb + flat // D) * D, D)
            pltpu.make_async_copy(own.at[rows, :], gbu.at[ds(flat % D, CR), cols], ou_sem).start()

        @pl.when(k >= K // 2)
        def _():
            flat = half * (FF // 2) + (k - K // 2) * CR
            pltpu.make_async_copy(own.at[rows, :], gbd.at[ds(flat, CR), :], od_sem).start()

    def z_step(i):
        @pl.when(i < K)
        def _():
            @pl.when(is_mid)
            def _():
                await_f32(gb_recv, ag_near, i)

            gb_copy(ag_near, i).start()
            gb_store(ag_near, i)

        k = i - lag

        @pl.when((k >= 0) & (k < K))
        def _():
            await_f32(gb_recv, ag_far, k)

            @pl.when(is_mid)
            def _():
                gb_copy(ag_far, k).start()

            gb_store(ag_far, k)

    def y_copy(u):
        return pltpu.make_async_remote_copy(ybuf.at[u % NS], xin.at[ds(u * UR, UR), :], y_send.at[u % NS], x_recv.at[u],
                                            device_id={"stage": s + 1}, device_id_type=MESH)

    def y_store(u):
        return pltpu.make_async_copy(ybuf.at[u % NS], ys.at[ds(u * UR, UR), :], y_out.at[u % NS])

    def y_drain(u):
        @pl.when(s < last)
        def _():
            y_copy(u).wait_send()

        y_store(u).wait()

    def unit(u):
        rows = ds(u * UR, UR)

        @pl.when(u >= NS)
        def _():
            y_drain(u - NS)

        pltpu.make_async_copy(xin.at[rows, :], xin.at[rows, :], x_recv.at[u]).wait()
        x = xin[rows, :]
        total = None
        for c in range(nblk):
            hid = gelu_tanh(mat(x, wbuf[ru(c):ru(c) + D, :])).astype(BF16)
            piece = mat(hid, wbuf[rv(c):rv(c) + D, :])
            total = piece if total is None else total + piece
        ybuf[u % NS] = (x.astype(F32) + total).astype(BF16)

        @pl.when(s < last)
        def _():
            y_copy(u).start()

        y_store(u).start()

    z_total = K + cfg.LAG_END
    z_pre = 2 * s

    @pl.loop(0, z_pre)
    def _(i):
        z_step(i)

    @pl.loop(0, NU)
    def _(u):
        unit(u)
        z_step(u + z_pre)

    @pl.loop(NU + z_pre, z_total)
    def _(i):
        z_step(i)

    @pl.loop(NU - NS, NU)
    def _(u):
        y_drain(u)

    @pl.when(s > 0)
    def _():
        @pl.loop(0, NB)
        def _(j):
            g_copy(j).wait_send()

    @pl.when(is_end)
    def _():
        @pl.loop(0, R * S)
        def _(dev):
            @pl.when(dev != me)
            def _():
                c_copy(dev).wait_send()

    @pl.loop(0, K)
    def _(k):
        w_copy(ag_near, k).wait_send()
        gb_copy(ag_near, k).wait_send()

        @pl.when(is_mid)
        def _():
            rs_copy(rbuf, rs_near, k).wait_send()
            rs_copy(rbuf, rs_far, k).wait_send()
            w_copy(ag_far, k).wait_send()
            gb_copy(ag_far, k).wait_send()

    pltpu.make_async_copy(gbu, gbu, ou_sem).wait()
    pltpu.make_async_copy(gbd, gbd, od_sem).wait()
    pltpu.make_async_copy(cvec, c_out, co_sem).wait()


def mega_call(cfg, lr, mn, acts, mu, md, dy, gu, gd, m1u, m1d, m2u, m2d, nb):
    D, FF, T, M = cfg.D, cfg.FF, cfg.T, cfg.M
    any_spec = pl.BlockSpec(memory_space=pl.ANY)
    smem = pl.BlockSpec(memory_space=pltpu.SMEM)
    dma = pltpu.SemaphoreType.DMA
    return pl.pallas_call(
        functools.partial(mega, cfg),
        out_shape=(
            jax.ShapeDtypeStruct((D, FF), F32),
            jax.ShapeDtypeStruct((FF, D), F32),
            jax.ShapeDtypeStruct((8, 128), F32),
            jax.ShapeDtypeStruct((M * T, D), BF16),
        ),
        in_specs=[smem, smem] + [any_spec] * 11,
        out_specs=(any_spec,) * 4,
        scratch_shapes=[
            pltpu.VMEM((2 * FF, D), F32),
            pltpu.VMEM((2 * FF, D), F32),
            pltpu.VMEM((2 * FF, D), BF16),
            pltpu.VMEM((M * T, D), BF16),
            pltpu.VMEM((cfg.NS, cfg.UR, D), BF16),
            pltpu.VMEM((T, D), BF16),
            pltpu.VMEM((T, D), BF16),
            pltpu.VMEM((2 * FF, D), F32),
            pltpu.VMEM((FF, D), BF16),
            pltpu.VMEM((FF, D), BF16),
            pltpu.VMEM((FF, T), BF16),
            pltpu.VMEM((cfg.nblk * T, D), BF16),
            pltpu.VMEM((max(cfg.nblk * T, FF), D), F32),
            pltpu.VMEM((FF, D), F32),
            pltpu.VMEM((T, D), BF16),
            pltpu.VMEM((D, T), BF16),
            pltpu.VMEM((8, D), F32),
            pltpu.VMEM((2 * cfg.S, 8, 128), F32),
            pltpu.VMEM((8, 128), F32),
            dma,
            dma((2 * cfg.nblk,)),
            dma((2 * cfg.nblk,)),
            dma((4 * cfg.hb,)),
            dma((cfg.NB,)),
            dma((cfg.NB,)),
            dma((2, cfg.K)),
            dma((2, cfg.K)),
            dma((2 * cfg.S,)),
            dma((cfg.R * cfg.S,)),
            dma((2, cfg.K)),
            dma((2, cfg.K)),
            dma((2, cfg.K)),
            dma((2, cfg.K)),
            dma((cfg.NU,)),
            dma((cfg.NS,)),
            dma((cfg.NS,)),
            dma,
            dma,
            dma,
        ],
        compiler_params=pltpu.CompilerParams(
            collective_id=0, has_side_effects=True, vmem_limit_bytes=67043328),
        name="pipeline_step",
    )(lr, mn, acts, mu, md, dy, gu, gd, m1u, m1d, m2u, m2d, nb)


def solution(mesh):
    n_stages = mesh.shape['stage']
    n_reps = mesh.shape['data']

    def local_step(master_up, master_down, mom1_up, mom1_down, mom2_up, mom2_down, grad_up, grad_down, stage_acts, loss_grad, next_batch, learn_rate, max_norm):
        n_micro, rows, width = next_batch.shape
        hidden = master_up.shape[2]
        cfg = Cfg(n_reps, n_stages, width, hidden, rows, n_micro)
        gbar_up, gbar_down, clip, outs = mega_call(
            cfg, learn_rate.reshape(1), max_norm.reshape(1), stage_acts[0], master_up[0], master_down[0], loss_grad,
            grad_up[0, 0], grad_down[0, 0], mom1_up[0], mom1_down[0], mom2_up[0], mom2_down[0],
            next_batch.reshape(n_micro * rows, width))
        clip_scale = clip[0, 0]
        new_up, new_m1_up, new_m2_up = adamw_update(master_up[0], mom1_up[0], mom2_up[0], gbar_up, clip_scale, learn_rate)
        new_down, new_m1_down, new_m2_down = adamw_update(master_down[0], mom1_down[0], mom2_down[0], gbar_down, clip_scale, learn_rate)
        stage_outs = outs.reshape(1, n_micro, rows, width)
        return (new_up[None], new_down[None], new_m1_up[None], new_m1_down[None], new_m2_up[None], new_m2_down[None], stage_outs)

    w_spec = P('stage', None, None)
    g_spec = P('data', 'stage', None, None)
    in_specs = (w_spec, w_spec, w_spec, w_spec, w_spec, w_spec, g_spec, g_spec, P('stage', 'data', None), P('data', None), P(None, 'data', None), P(), P())
    out_specs = (w_spec, w_spec, w_spec, w_spec, w_spec, w_spec, P('stage', None, 'data', None))
    return jax.shard_map(local_step, mesh=mesh, in_specs=in_specs, out_specs=out_specs, check_vma=False)
```

```python
import functools

import jax
import jax.numpy as jnp
from jax import lax
from jax.experimental import pallas as pl
from jax.experimental.pallas import tpu as pltpu
from jax.sharding import PartitionSpec as P

BETA1 = 0.9
BETA2 = 0.95
ADAM_EPS = 1e-8
WEIGHT_DECAY = 0.1
NORM_EPS = 1e-6
ADAM_STEP = 8
SQRT_TWO_PI = 0.7978845608028654
GELU_CUBIC = 0.044715

MESH = pl.DeviceIdType.MESH
F32 = jnp.float32
BF16 = jnp.bfloat16


def tanh_part(pre_act):
    return jnp.tanh(SQRT_TWO_PI * (pre_act + GELU_CUBIC * pre_act * pre_act * pre_act))


def gelu_tanh(pre_act):
    return 0.5 * pre_act * (1.0 + tanh_part(pre_act))


def gelu_pair(pre_act):
    tanh_val = tanh_part(pre_act)
    act_value = 0.5 * pre_act * (1.0 + tanh_val)
    act_slope = 0.5 * (1.0 + tanh_val) + 0.5 * pre_act * (1.0 - tanh_val * tanh_val) * SQRT_TWO_PI * (1.0 + 3.0 * GELU_CUBIC * pre_act * pre_act)
    return act_value, act_slope


def mat(left, right):
    return jnp.dot(left, right, preferred_element_type=F32)


def mat_nt(left, right):
    return lax.dot_general(left, right, (((1,), (1,)), ((), ())), preferred_element_type=F32)


def adamw_update(master, first_mom, second_mom, grad_avg, clip_scale, learn_rate):
    scaled = clip_scale * grad_avg
    new_first = BETA1 * first_mom + (1.0 - BETA1) * scaled
    new_second = BETA2 * second_mom + (1.0 - BETA2) * scaled * scaled
    first_hat = new_first / (1.0 - BETA1 ** ADAM_STEP)
    second_hat = new_second / (1.0 - BETA2 ** ADAM_STEP)
    new_master = master - learn_rate * (first_hat / (jnp.sqrt(second_hat) + ADAM_EPS) + WEIGHT_DECAY * master)
    return new_master, new_first, new_second


class Cfg:
    def __init__(self, reps, stages, width, hidden, rows, micro):
        self.R, self.S, self.D, self.FF, self.T, self.M = reps, stages, width, hidden, rows, micro
        self.nblk = hidden // width
        self.hb = self.nblk // 2
        self.NB = 4
        self.BR = rows // self.NB
        self.CR = width // 8
        self.K = hidden // self.CR
        self.UR = rows // 4
        self.NU = micro * rows // self.UR
        self.NS = 16
        self.LAG_MID = 2
        self.LAG_END = 8


def mega(cfg, lr_ref, mn_ref, acts, mu, md, dy, gu, gd, m1u, m1d, m2u, m2d, nb,
         gbu, gbd, c_out, ys,
         own, rbuf, wbuf, xin, ybuf, gin, gout, muf, ubf, vbf, ubt, vbt, ht, dpre, slope, m2b, av, at, sq, cbuf, cvec,
         ld_sem, ldw_sem, ldg_sem, ldm_sem, g_recv, g_send, rs_recv, rs_send, c_recv, c_send, w_recv, w_send,
         gb_recv, gb_send, x_recv, y_send, y_out, ou_sem, od_sem, co_sem):
    R, S, D, FF, T, M = cfg.R, cfg.S, cfg.D, cfg.FF, cfg.T, cfg.M
    nblk, hb, NB, BR, CR, K, UR, NU, NS = cfg.nblk, cfg.hb, cfg.NB, cfg.BR, cfg.CR, cfg.K, cfg.UR, cfg.NU, cfg.NS
    r = lax.axis_index("data")
    s = lax.axis_index("stage")
    last = S - 1
    is_end = (r == 0) | (r == R - 1)
    is_mid = jnp.logical_not(is_end)
    low = r < R // 2

    def ru(c):
        return (c // hb) * FF + (c % hb) * D

    def rv(c):
        return ru(c) + FF // 2

    def ds(start, size):
        return pl.ds(pl.multiple_of(start, size), size)

    barrier = pltpu.get_barrier_semaphore()

    @pl.loop(0, R * S)
    def _(dev):
        pl.semaphore_signal(barrier, inc=1, device_id=(dev // S, dev % S), device_id_type=MESH)

    act_load = pltpu.make_async_copy(acts, av, ld_sem)
    act_load.start()
    w_loads = []
    for c in range(nblk):
        w_loads.append(pltpu.make_async_copy(mu.at[:, c * D:(c + 1) * D], muf.at[ru(c):ru(c) + D, :], ldw_sem.at[c]))
    for c in range(nblk):
        w_loads.append(pltpu.make_async_copy(md.at[c * D:(c + 1) * D, :], muf.at[rv(c):rv(c) + D, :], ldw_sem.at[nblk + c]))
    for load in w_loads:
        load.start()

    @pl.when(s == last)
    def _():
        for j in range(NB):
            pltpu.make_async_copy(dy.at[j * BR:(j + 1) * BR, :], gin.at[j * BR:(j + 1) * BR, :], g_recv.at[j]).start()

    g_loads = []
    for c in range(nblk):
        g_loads.append(pltpu.make_async_copy(gu.at[:, c * D:(c + 1) * D], own.at[ru(c):ru(c) + D, :], ldg_sem.at[c]))
        g_loads.append(pltpu.make_async_copy(gd.at[c * D:(c + 1) * D, :], own.at[rv(c):rv(c) + D, :], ldg_sem.at[nblk + c]))

    act_load.wait()
    for c in range(nblk):
        w_loads[c].wait()
        ubf[c * D:(c + 1) * D, :] = muf[ru(c):ru(c) + D, :].astype(BF16)

    for c in range(nblk):
        w_loads[nblk + c].wait()
        vbf[c * D:(c + 1) * D, :] = muf[rv(c):rv(c) + D, :].astype(BF16)
    for load in g_loads:
        load.start()

    late = s >= S - 2

    def slope_part(j):
        for c in range(nblk):
            pre = mat(av[ds(j * BR, BR), :], ubf[c * D:(c + 1) * D, :])
            _, act_slope = gelu_pair(pre)
            slope[ds(c * T + j * BR, BR), :] = act_slope

    def hidden_part(j):
        @pl.loop(0, nblk)
        def _(c):
            pre = mat(av[ds(j * BR, BR), :], ubf[ds(c * D, D), :])
            ht[ds(c * D, D), ds(j * BR, BR)] = gelu_tanh(pre).T.astype(BF16)

    def transpose_acts():
        at[...] = av[...].astype(F32).T.astype(BF16)

    @pl.when(s < last)
    def _():
        @pl.loop(0, nblk)
        def _(c):
            rows = ds(c * D, D)
            ubt[rows, :] = ubf[rows, :].T
            vbt[rows, :] = vbf[rows, :].T

    @pl.when(jnp.logical_not(late))
    def _():
        @pl.loop(0, NB)
        def _(j):
            slope_part(j)

        @pl.loop(0, NB)
        def _(j):
            hidden_part(j)

        transpose_acts()

    @pl.when(s == 0)
    def _():
        @pl.loop(0, NU)
        def _(u):
            pltpu.make_async_copy(nb.at[ds(u * UR, UR), :], xin.at[ds(u * UR, UR), :], x_recv.at[u]).start()

    with jax.named_scope("barrier_wait"):
        pl.semaphore_wait(barrier, R * S)

    def g_copy(j):
        rows = ds(j * BR, BR)
        return pltpu.make_async_remote_copy(gout.at[rows, :], gin.at[rows, :], g_send.at[j], g_recv.at[j],
                                            device_id={"stage": s - 1}, device_id_type=MESH)

    def chain_step(j, down_of, up_of):
        rows = ds(j * BR, BR)
        g = gin[rows, :]
        total = None
        for c in range(nblk):
            part = ds(c * T + j * BR, BR)
            d_pre = (down_of(g, c) * slope[part, :]).astype(BF16)
            dpre[part, :] = d_pre
            if up_of is not None:
                piece = up_of(d_pre, c)
                total = piece if total is None else total + piece
        if up_of is not None:
            gout[rows, :] = (g.astype(F32) + total).astype(BF16)
            g_copy(j).start()

    def chain_wait(j):
        rows = ds(j * BR, BR)
        with jax.named_scope("chain_wait"):
            pltpu.make_async_copy(gin.at[rows, :], gin.at[rows, :], g_recv.at[j]).wait()

    @pl.when(s == last)
    def _():
        @pl.loop(0, NB)
        def _(j):
            slope_part(j)
            chain_wait(j)
            chain_step(j, lambda g, c: mat_nt(g, vbf[c * D:(c + 1) * D, :]), lambda d, c: mat_nt(d, ubf[c * D:(c + 1) * D, :]))

    @pl.when(s < last)
    def _():
        @pl.loop(0, NB)
        def _(j):
            @pl.when(late)
            def _():
                slope_part(j)

            chain_wait(j)

            @pl.when(s > 0)
            def _():
                chain_step(j, lambda g, c: mat(g, vbt[c * D:(c + 1) * D, :]), lambda d, c: mat(d, ubt[c * D:(c + 1) * D, :]))

            @pl.when(s == 0)
            def _():
                chain_step(j, lambda g, c: mat(g, vbt[c * D:(c + 1) * D, :]), None)

    @pl.when(late)
    def _():
        @pl.loop(0, NB)
        def _(j):
            hidden_part(j)

        transpose_acts()

    for load in g_loads:
        load.wait()

    half_d = D // 2

    def add_weight_grads(j):
        @pl.when(j < hb)
        def _():
            for half in (0, 1):
                for m in (0, 1):
                    rows = ds(half * FF + j * D + m * half_d, half_d)
                    own[rows, :] += mat(at[m * half_d:(m + 1) * half_d, :], dpre[ds((half * hb + j) * T, T), :])

        @pl.when(j >= hb)
        def _():
            for half in (0, 1):
                for m in (0, 1):
                    rows = ds(half * FF + j * D + m * half_d, half_d)
                    own[rows, :] += mat(ht[ds((half * hb + j - hb) * D + m * half_d, half_d), :], gin[...])

    def moment_loads(half):
        out = []
        for b in range(hb):
            cols = slice((half * hb + b) * D, (half * hb + b + 1) * D)
            out.append(pltpu.make_async_copy(m1u.at[:, cols], slope.at[b * D:(b + 1) * D, :], ldm_sem.at[b]))
            out.append(pltpu.make_async_copy(m2u.at[:, cols], m2b.at[b * D:(b + 1) * D, :], ldm_sem.at[hb + b]))
            out.append(pltpu.make_async_copy(m1d.at[cols, :], slope.at[FF // 2 + b * D:FF // 2 + (b + 1) * D, :], ldm_sem.at[2 * hb + b]))
            out.append(pltpu.make_async_copy(m2d.at[cols, :], m2b.at[FF // 2 + b * D:FF // 2 + (b + 1) * D, :], ldm_sem.at[3 * hb + b]))
        return out

    for half, where in ((0, r == 0), (1, r == R - 1)):
        @pl.when(where)
        def _():
            for load in moment_loads(half):
                load.start()

    def half_rows(half, k):
        return ds(half * FF + k * CR, CR)

    def await_f32(sem, half, k):
        rows = half_rows(half, k)
        pltpu.make_async_copy(own.at[rows, :], own.at[rows, :], sem.at[half, k]).wait()

    def rs_copy(src, half, k):
        rows = half_rows(half, k)
        return pltpu.make_async_remote_copy(src.at[rows, :], rbuf.at[rows, :], rs_send.at[half], rs_recv.at[half, k],
                                            device_id={"data": r + 2 * half - 1}, device_id_type=MESH)

    def half_sent(ref, sem, half):
        rows = ds(half * FF, FF)
        pltpu.make_async_copy(ref.at[rows, :], ref.at[rows, :], sem.at[half]).wait()

    rs_near = jnp.where(low, 1, 0)
    rs_far = 1 - rs_near
    lag = jnp.where(is_end, cfg.LAG_END, cfg.LAG_MID)
    sq[...] = jnp.zeros_like(sq)

    per_block = D // CR

    @pl.loop(0, K + cfg.LAG_END)
    def _(i):
        @pl.when((i % per_block == 0) & (i < K))
        def _():
            with jax.named_scope("weight_grads"):
                add_weight_grads(i // per_block)

        @pl.when((i < K) & is_end)
        def _():
            rs_copy(own, rs_near, i).start()

        @pl.when((i < K) & is_mid)
        def _():
            await_f32(rs_recv, rs_near, i)
            rows = half_rows(rs_near, i)
            rbuf[rows, :] += own[rows, :]
            rs_copy(rbuf, rs_near, i).start()

        k = i - lag

        @pl.when((k >= 0) & (k < K) & is_mid)
        def _():
            with jax.named_scope("rs_far_wait"):
                await_f32(rs_recv, rs_far, k)
            rows = half_rows(rs_far, k)
            rbuf[rows, :] += own[rows, :]
            rs_copy(rbuf, rs_far, k).start()

        @pl.when((k >= 0) & (k < K) & is_end)
        def _():
            with jax.named_scope("rs_end_wait"):
                await_f32(rs_recv, rs_far, k)
            rows = half_rows(rs_far, k)
            mean = (own[rows, :] + rbuf[rows, :]) * (1.0 / R)
            own[rows, :] = mean
            sq[...] += jnp.sum((mean * mean).reshape(CR // 8, 8, D), axis=0)

    mine = jnp.where(r == 0, s, S + s)
    me = r * S + s

    def c_copy(dev):
        return pltpu.make_async_remote_copy(cbuf.at[mine], cbuf.at[mine], c_send, c_recv.at[mine],
                                            device_id=(dev // S, dev % S), device_id_type=MESH)

    @pl.when(is_end)
    def _():
        part = sq[:, 0:128]
        for q in range(1, D // 128):
            part = part + sq[:, q * 128:(q + 1) * 128]
        cbuf[mine] = part

        half_sent(own, rs_send, rs_near)

        @pl.loop(0, R * S)
        def _(dev):
            @pl.when(dev != me)
            def _():
                c_copy(dev).start()

    with jax.named_scope("clip_wait"):
        @pl.loop(0, 2 * S)
        def _(slot):
            @pl.when(is_mid | (slot != mine))
            def _():
                pltpu.make_async_copy(cbuf.at[slot], cbuf.at[slot], c_recv.at[slot]).wait()

    total_sq = cbuf[0]
    for slot in range(1, 2 * S):
        total_sq = total_sq + cbuf[slot]
    total_sq = jnp.sum(jnp.sum(total_sq, axis=0, keepdims=True), axis=1, keepdims=True)
    grad_norm = jnp.sqrt(jnp.broadcast_to(total_sq, (8, 128)))
    cvec[...] = jnp.minimum(1.0, mn_ref[0] / (grad_norm + NORM_EPS))
    pltpu.make_async_copy(cvec, c_out, co_sem).start()

    for half, where in ((0, r == 0), (1, r == R - 1)):
        @pl.when(where)
        def _():
            for load in moment_loads(half):
                load.wait()

    ag_near = 1 - rs_near
    ag_far = rs_near

    def w_copy(half, k):
        rows = half_rows(half, k)
        return pltpu.make_async_remote_copy(wbuf.at[rows, :], wbuf.at[rows, :], w_send.at[half], w_recv.at[half, k],
                                            device_id={"data": r + 1 - 2 * half}, device_id_type=MESH)

    def await_w(half, k):
        rows = half_rows(half, k)
        pltpu.make_async_copy(wbuf.at[rows, :], wbuf.at[rows, :], w_recv.at[half, k]).wait()

    @pl.loop(0, K + cfg.LAG_MID)
    def _(i):
        @pl.when((i < K) & is_end)
        def _():
            rows = half_rows(ag_near, i)
            local = ds(i * CR, CR)
            clip = cvec[0:1, 0:1]
            new_master, _, _ = adamw_update(muf[rows, :], slope[local, :], m2b[local, :], own[rows, :], clip, lr_ref[0])
            wbuf[rows, :] = new_master.astype(BF16)
            w_copy(ag_near, i).start()

        @pl.when((i < K) & is_mid)
        def _():
            with jax.named_scope("w_near_wait"):
                await_w(ag_near, i)
            w_copy(ag_near, i).start()

        k = i - cfg.LAG_MID

        @pl.when((k >= 0) & is_mid)
        def _():
            await_w(ag_far, k)
            w_copy(ag_far, k).start()

    def gb_copy(half, k):
        rows = half_rows(half, k)
        return pltpu.make_async_remote_copy(own.at[rows, :], own.at[rows, :], gb_send.at[half], gb_recv.at[half, k],
                                            device_id={"data": r + 1 - 2 * half}, device_id_type=MESH)

    def gb_store(half, k):
        rows = half_rows(half, k)

        @pl.when(k < K // 2)
        def _():
            flat = k * CR
            cols = ds((half * hb + flat // D) * D, D)
            pltpu.make_async_copy(own.at[rows, :], gbu.at[ds(flat % D, CR), cols], ou_sem).start()

        @pl.when(k >= K // 2)
        def _():
            flat = half * (FF // 2) + (k - K // 2) * CR
            pltpu.make_async_copy(own.at[rows, :], gbd.at[ds(flat, CR), :], od_sem).start()

    def z_step(i):
        @pl.when(i < K)
        def _():
            @pl.when(is_mid)
            def _():
                await_f32(gb_recv, ag_near, i)
                gb_copy(ag_near, i).start()

            gb_store(ag_near, i)

        k = i - lag

        @pl.when((k >= 0) & (k < K))
        def _():
            await_f32(gb_recv, ag_far, k)

            @pl.when(is_mid)
            def _():
                gb_copy(ag_far, k).start()

            gb_store(ag_far, k)

    @pl.when(is_end)
    def _():
        @pl.loop(0, K)
        def _(k):
            gb_copy(ag_near, k).start()

        @pl.loop(0, K)
        def _(k):
            with jax.named_scope("w_end_wait"):
                await_w(ag_far, k)

    def y_copy(u):
        return pltpu.make_async_remote_copy(ybuf.at[u % NS], xin.at[ds(u * UR, UR), :], y_send.at[u % NS], x_recv.at[u],
                                            device_id={"stage": s + 1}, device_id_type=MESH)

    def y_store(u):
        return pltpu.make_async_copy(ybuf.at[u % NS], ys.at[ds(u * UR, UR), :], y_out.at[u % NS])

    def y_drain(u):
        @pl.when(s < last)
        def _():
            y_copy(u).wait_send()

        y_store(u).wait()

    def unit(u):
        rows = ds(u * UR, UR)

        @pl.when(u >= NS)
        def _():
            with jax.named_scope("y_wait"):
                y_drain(u - NS)

        with jax.named_scope("x_wait"):
            pltpu.make_async_copy(xin.at[rows, :], xin.at[rows, :], x_recv.at[u]).wait()
        x = xin[rows, :]
        total = None
        for c in range(nblk):
            hid = gelu_tanh(mat(x, wbuf[ru(c):ru(c) + D, :])).astype(BF16)
            piece = mat(hid, wbuf[rv(c):rv(c) + D, :])
            total = piece if total is None else total + piece
        ybuf[u % NS] = (x.astype(F32) + total).astype(BF16)

        @pl.when(s < last)
        def _():
            y_copy(u).start()

        y_store(u).start()

    z_total = K + cfg.LAG_END
    z_pre = s - 1

    with jax.named_scope("z_pre"):
        @pl.loop(0, z_pre)
        def _(i):
            z_step(i)

    @pl.loop(0, NU)
    def _(u):
        unit(u)

        @pl.when((u % 2 == 1) & (u // 2 + z_pre >= 0))
        def _():
            with jax.named_scope("z_step"):
                z_step(u // 2 + z_pre)

    with jax.named_scope("z_tail"):
        @pl.loop(NU // 2 + z_pre, z_total)
        def _(i):
            z_step(i)

    @pl.loop(NU - NS, NU)
    def _(u):
        y_drain(u)

    @pl.when(s > 0)
    def _():
        @pl.loop(0, NB)
        def _(j):
            g_copy(j).wait_send()

    @pl.when(is_end)
    def _():
        pltpu.make_async_copy(cbuf.at[0:R * S - 1], cbuf.at[0:R * S - 1], c_send).wait()

    half_sent(wbuf, w_send, ag_near)
    half_sent(own, gb_send, ag_near)

    @pl.when(is_mid)
    def _():
        half_sent(rbuf, rs_send, rs_near)
        half_sent(rbuf, rs_send, rs_far)
        half_sent(wbuf, w_send, ag_far)
        half_sent(own, gb_send, ag_far)

    pltpu.make_async_copy(gbu, gbu, ou_sem).wait()
    pltpu.make_async_copy(gbd, gbd, od_sem).wait()
    pltpu.make_async_copy(cvec, c_out, co_sem).wait()


def mega_call(cfg, lr, mn, acts, mu, md, dy, gu, gd, m1u, m1d, m2u, m2d, nb):
    D, FF, T, M = cfg.D, cfg.FF, cfg.T, cfg.M
    any_spec = pl.BlockSpec(memory_space=pl.ANY)
    smem = pl.BlockSpec(memory_space=pltpu.SMEM)
    dma = pltpu.SemaphoreType.DMA
    return pl.pallas_call(
        functools.partial(mega, cfg),
        out_shape=(
            jax.ShapeDtypeStruct((D, FF), F32),
            jax.ShapeDtypeStruct((FF, D), F32),
            jax.ShapeDtypeStruct((8, 128), F32),
            jax.ShapeDtypeStruct((M * T, D), BF16),
        ),
        in_specs=[smem, smem] + [any_spec] * 11,
        out_specs=(any_spec,) * 4,
        scratch_shapes=[
            pltpu.VMEM((2 * FF, D), F32),
            pltpu.VMEM((2 * FF, D), F32),
            pltpu.VMEM((2 * FF, D), BF16),
            pltpu.VMEM((M * T, D), BF16),
            pltpu.VMEM((cfg.NS, cfg.UR, D), BF16),
            pltpu.VMEM((T, D), BF16),
            pltpu.VMEM((T, D), BF16),
            pltpu.VMEM((2 * FF, D), F32),
            pltpu.VMEM((FF, D), BF16),
            pltpu.VMEM((FF, D), BF16),
            pltpu.VMEM((FF, D), BF16),
            pltpu.VMEM((FF, D), BF16),
            pltpu.VMEM((FF, T), BF16),
            pltpu.VMEM((cfg.nblk * T, D), BF16),
            pltpu.VMEM((max(cfg.nblk * T, FF), D), F32),
            pltpu.VMEM((FF, D), F32),
            pltpu.VMEM((T, D), BF16),
            pltpu.VMEM((D, T), BF16),
            pltpu.VMEM((8, D), F32),
            pltpu.VMEM((cfg.R * cfg.S, 8, 128), F32),
            pltpu.VMEM((8, 128), F32),
            dma,
            dma((2 * cfg.nblk,)),
            dma((2 * cfg.nblk,)),
            dma((4 * cfg.hb,)),
            dma((cfg.NB,)),
            dma((cfg.NB,)),
            dma((2, cfg.K)),
            dma((2,)),
            dma((2 * cfg.S,)),
            dma,
            dma((2, cfg.K)),
            dma((2,)),
            dma((2, cfg.K)),
            dma((2,)),
            dma((cfg.NU,)),
            dma((cfg.NS,)),
            dma((cfg.NS,)),
            dma,
            dma,
            dma,
        ],
        compiler_params=pltpu.CompilerParams(
            collective_id=0, has_side_effects=True, vmem_limit_bytes=67043328),
        name="pipeline_step",
    )(lr, mn, acts, mu, md, dy, gu, gd, m1u, m1d, m2u, m2d, nb)


def finish(steps, lr_ref, clip_ref, gu, gd, mu, md, m1u, m1d, m2u, m2d, rows_in,
           new_u, new_d, new_m1u, new_m1d, new_m2u, new_m2d, rows_out,
           guv, gdv, muv, mdv, m1uv, m1dv, m2uv, m2dv, rv, in_sem, out_sem):
    reads = ((gu, guv), (mu, muv), (m1u, m1uv), (m2u, m2uv), (gd, gdv), (md, mdv), (m1d, m1dv), (m2d, m2dv), (rows_in, rv))
    writes = ((muv, new_u), (m1uv, new_m1u), (m2uv, new_m2u), (mdv, new_d), (m1dv, new_m1d), (m2dv, new_m2d), (rv, rows_out))

    def part(x, i):
        size = x.shape[0] // steps
        return pl.ds(pl.multiple_of(i * size, size), size)

    def read(n, i):
        src, dst = reads[n]
        return pltpu.make_async_copy(src.at[part(src, i), :], dst.at[part(src, i), :], in_sem.at[n, i])

    def write(n, i):
        src, dst = writes[n]
        return pltpu.make_async_copy(src.at[part(src, i), :], dst.at[part(src, i), :], out_sem.at[n])

    @pl.loop(0, steps)
    def _(i):
        for n in range(len(reads)):
            read(n, i).start()

    clip = clip_ref[0:1, 0:1]

    @pl.loop(0, steps)
    def _(i):
        for g, w, m1, m2, first, out in ((guv, muv, m1uv, m2uv, 0, 0), (gdv, mdv, m1dv, m2dv, 4, 3)):
            for n in range(first, first + 4):
                read(n, i).wait()
            p = part(g, i)
            w[p, :], m1[p, :], m2[p, :] = adamw_update(w[p, :], m1[p, :], m2[p, :], g[p, :], clip, lr_ref[0])
            for n in range(out, out + 3):
                write(n, i).start()
        read(8, i).wait()
        write(6, i).start()

    for n in range(len(writes)):
        pltpu.make_async_copy(writes[n][0], writes[n][1], out_sem.at[n]).wait()


def finish_call(lr, clip, gu, gd, mu, md, m1u, m1d, m2u, m2d, rows_in, steps):
    ins = (gu, gd, mu, md, m1u, m1d, m2u, m2d, rows_in)
    outs = (mu, md, m1u, m1d, m2u, m2d, rows_in)
    any_spec = pl.BlockSpec(memory_space=pl.ANY)
    return pl.pallas_call(
        functools.partial(finish, steps),
        out_shape=tuple(jax.ShapeDtypeStruct(x.shape, x.dtype) for x in outs),
        in_specs=[pl.BlockSpec(memory_space=pltpu.SMEM), pl.BlockSpec(memory_space=pltpu.VMEM)] + [any_spec] * len(ins),
        out_specs=(any_spec,) * len(outs),
        scratch_shapes=[pltpu.VMEM(x.shape, x.dtype) for x in ins]
        + [pltpu.SemaphoreType.DMA((len(ins), steps)), pltpu.SemaphoreType.DMA((len(outs),))],
        compiler_params=pltpu.CompilerParams(vmem_limit_bytes=67043328),
        name="finish",
    )(lr, clip, *ins)


def solution(mesh):
    n_stages = mesh.shape['stage']
    n_reps = mesh.shape['data']

    def local_step(master_up, master_down, mom1_up, mom1_down, mom2_up, mom2_down, grad_up, grad_down, stage_acts, loss_grad, next_batch, learn_rate, max_norm):
        n_micro, rows, width = next_batch.shape
        hidden = master_up.shape[2]
        cfg = Cfg(n_reps, n_stages, width, hidden, rows, n_micro)
        gbar_up, gbar_down, clip, outs = mega_call(
            cfg, learn_rate.reshape(1), max_norm.reshape(1), stage_acts[0], master_up[0], master_down[0], loss_grad,
            grad_up[0, 0], grad_down[0, 0], mom1_up[0], mom1_down[0], mom2_up[0], mom2_down[0],
            next_batch.reshape(n_micro * rows, width))
        new_up, new_down, new_m1_up, new_m1_down, new_m2_up, new_m2_down, outs = finish_call(
            learn_rate.reshape(1), clip, gbar_up, gbar_down, master_up[0], master_down[0], mom1_up[0], mom1_down[0],
            mom2_up[0], mom2_down[0], outs, 16)
        stage_outs = outs.reshape(1, n_micro, rows, width)
        return (new_up[None], new_down[None], new_m1_up[None], new_m1_down[None], new_m2_up[None], new_m2_down[None], stage_outs)

    w_spec = P('stage', None, None)
    g_spec = P('data', 'stage', None, None)
    in_specs = (w_spec, w_spec, w_spec, w_spec, w_spec, w_spec, g_spec, g_spec, P('stage', 'data', None), P('data', None), P(None, 'data', None), P(), P())
    out_specs = (w_spec, w_spec, w_spec, w_spec, w_spec, w_spec, P('stage', None, 'data', None))
    return jax.shard_map(local_step, mesh=mesh, in_specs=in_specs, out_specs=out_specs, check_vma=False)
```

```python
import functools

import jax
import jax.numpy as jnp
from jax import lax
from jax.experimental import pallas as pl
from jax.experimental.pallas import tpu as pltpu
from jax.sharding import PartitionSpec as P

BETA1 = 0.9
BETA2 = 0.95
ADAM_EPS = 1e-8
WEIGHT_DECAY = 0.1
NORM_EPS = 1e-6
ADAM_STEP = 8
SQRT_TWO_PI = 0.7978845608028654
GELU_CUBIC = 0.044715

MESH = pl.DeviceIdType.MESH
F32 = jnp.float32
BF16 = jnp.bfloat16


def tanh_part(pre_act):
    return jnp.tanh(SQRT_TWO_PI * (pre_act + GELU_CUBIC * pre_act * pre_act * pre_act))


def gelu_tanh(pre_act):
    return 0.5 * pre_act * (1.0 + tanh_part(pre_act))


def gelu_pair(pre_act):
    tanh_val = tanh_part(pre_act)
    act_value = 0.5 * pre_act * (1.0 + tanh_val)
    act_slope = 0.5 * (1.0 + tanh_val) + 0.5 * pre_act * (1.0 - tanh_val * tanh_val) * SQRT_TWO_PI * (1.0 + 3.0 * GELU_CUBIC * pre_act * pre_act)
    return act_value, act_slope


def mat(left, right):
    return jnp.dot(left, right, preferred_element_type=F32)


def mat_nt(left, right):
    return lax.dot_general(left, right, (((1,), (1,)), ((), ())), preferred_element_type=F32)


def adamw_update(master, first_mom, second_mom, grad_avg, clip_scale, learn_rate):
    scaled = clip_scale * grad_avg
    new_first = BETA1 * first_mom + (1.0 - BETA1) * scaled
    new_second = BETA2 * second_mom + (1.0 - BETA2) * scaled * scaled
    first_hat = new_first / (1.0 - BETA1 ** ADAM_STEP)
    second_hat = new_second / (1.0 - BETA2 ** ADAM_STEP)
    new_master = master - learn_rate * (first_hat / (jnp.sqrt(second_hat) + ADAM_EPS) + WEIGHT_DECAY * master)
    return new_master, new_first, new_second


class Cfg:
    def __init__(self, reps, stages, width, hidden, rows, micro):
        self.R, self.S, self.D, self.FF, self.T, self.M = reps, stages, width, hidden, rows, micro
        self.nblk = hidden // width
        self.hb = self.nblk // 2
        self.NB = 4
        self.BR = rows // self.NB
        self.CR = width // 16
        self.K = hidden // self.CR
        self.CG = width // 8
        self.KG = hidden // self.CG
        self.UR = rows // 4
        self.NU = micro * rows // self.UR
        self.NS = 16
        self.LAG_MID = 3
        self.LAG_END = 16
        self.GLAG_MID = 2
        self.GLAG_END = 8


def mega(cfg, lr_ref, mn_ref, acts, mu, md, dy, gu, gd, m1u, m1d, m2u, m2d, nb,
         gbu, gbd, c_out, ys,
         own, rbuf, wbuf, xin, ybuf, gin, gout, slope, mst, av, at, sq, cbuf, cvec,
         ld_sem, ldw_sem, ldg_sem, ldm_sem, g_recv, g_send, rs_recv, rs_send, c_recv, c_send, w_send,
         gb_recv, gb_send, x_recv, y_send, y_out, ou_sem, od_sem, co_sem):
    R, S, D, FF, T, M = cfg.R, cfg.S, cfg.D, cfg.FF, cfg.T, cfg.M
    CG, KG = cfg.CG, cfg.KG
    nblk, hb, NB, BR, CR, K, UR, NU, NS = cfg.nblk, cfg.hb, cfg.NB, cfg.BR, cfg.CR, cfg.K, cfg.UR, cfg.NU, cfg.NS
    r = lax.axis_index("data")
    s = lax.axis_index("stage")
    last = S - 1
    is_end = (r == 0) | (r == R - 1)
    is_mid = jnp.logical_not(is_end)
    low = r < R // 2

    UB, VB, UT, VT = 0, FF, 2 * FF, 3 * FF
    HT, DP = 0, FF

    def ru(c):
        return (c // hb) * FF + (c % hb) * D

    def rv(c):
        return ru(c) + FF // 2

    def ds(start, size):
        return pl.ds(pl.multiple_of(start, size), size)

    barrier = pltpu.get_barrier_semaphore()

    @pl.loop(0, R * S)
    def _(dev):
        pl.semaphore_signal(barrier, inc=1, device_id=(dev // S, dev % S), device_id_type=MESH)

    act_load = pltpu.make_async_copy(acts, av, ld_sem)
    act_load.start()
    w_loads = []
    for c in range(nblk):
        w_loads.append(pltpu.make_async_copy(mu.at[:, c * D:(c + 1) * D], own.at[ru(c):ru(c) + D, :], ldw_sem.at[c]))
    for c in range(nblk):
        w_loads.append(pltpu.make_async_copy(md.at[c * D:(c + 1) * D, :], own.at[rv(c):rv(c) + D, :], ldw_sem.at[nblk + c]))
    for load in w_loads:
        load.start()

    @pl.when(s == last)
    def _():
        for j in range(NB):
            pltpu.make_async_copy(dy.at[j * BR:(j + 1) * BR, :], gin.at[j * BR:(j + 1) * BR, :], g_recv.at[j]).start()

    g_loads = []
    for c in range(nblk):
        g_loads.append(pltpu.make_async_copy(gu.at[:, c * D:(c + 1) * D], own.at[ru(c):ru(c) + D, :], ldg_sem))
        g_loads.append(pltpu.make_async_copy(gd.at[c * D:(c + 1) * D, :], own.at[rv(c):rv(c) + D, :], ldg_sem))

    act_load.wait()
    for c in range(nblk):
        w_loads[c].wait()
        xin[UB + c * D:UB + (c + 1) * D, :] = own[ru(c):ru(c) + D, :].astype(BF16)

    for c in range(nblk):
        w_loads[nblk + c].wait()
        xin[VB + c * D:VB + (c + 1) * D, :] = own[rv(c):rv(c) + D, :].astype(BF16)
    for load in g_loads:
        load.start()

    late = s >= S // 2

    def slope_part(j):
        for c in range(nblk):
            pre = mat(av[ds(j * BR, BR), :], xin[UB + c * D:UB + (c + 1) * D, :])
            _, act_slope = gelu_pair(pre)
            slope[ds(c * T + j * BR, BR), :] = act_slope

    def hidden_part(j):
        @pl.loop(0, nblk)
        def _(c):
            pre = mat(av[ds(j * BR, BR), :], xin[ds(UB + c * D, D), :])
            wbuf[ds(HT + c * D, D), ds(j * BR, BR)] = gelu_tanh(pre).T.astype(BF16)

    def transpose_acts():
        at[...] = av[...].astype(F32).T.astype(BF16)

    @pl.when(s < last)
    def _():
        @pl.loop(0, nblk)
        def _(c):
            xin[ds(UT + c * D, D), :] = xin[ds(UB + c * D, D), :].T
            xin[ds(VT + c * D, D), :] = xin[ds(VB + c * D, D), :].T

    @pl.when(jnp.logical_not(late))
    def _():
        @pl.loop(0, NB)
        def _(j):
            slope_part(j)

        @pl.loop(0, NB)
        def _(j):
            hidden_part(j)

        transpose_acts()

    with jax.named_scope("barrier_wait"):
        pl.semaphore_wait(barrier, R * S)

    def g_copy(j):
        rows = ds(j * BR, BR)
        return pltpu.make_async_remote_copy(gout.at[rows, :], gin.at[rows, :], g_send.at[j], g_recv.at[j],
                                            device_id={"stage": s - 1}, device_id_type=MESH)

    def chain_step(j, down_of, up_of):
        rows = ds(j * BR, BR)
        g = gin[rows, :]
        total = None
        for c in range(nblk):
            part = ds(c * T + j * BR, BR)
            d_pre = (down_of(g, c) * slope[part, :]).astype(BF16)
            wbuf[ds(DP + c * T + j * BR, BR), :] = d_pre
            if up_of is not None:
                piece = up_of(d_pre, c)
                total = piece if total is None else total + piece
        if up_of is not None:
            gout[rows, :] = (g.astype(F32) + total).astype(BF16)
            g_copy(j).start()

    def chain_wait(j):
        rows = ds(j * BR, BR)
        with jax.named_scope("chain_wait"):
            pltpu.make_async_copy(gin.at[rows, :], gin.at[rows, :], g_recv.at[j]).wait()

    @pl.when(s == last)
    def _():
        @pl.loop(0, NB)
        def _(j):
            slope_part(j)
            chain_wait(j)
            chain_step(j, lambda g, c: mat_nt(g, xin[VB + c * D:VB + (c + 1) * D, :]),
                       lambda d, c: mat_nt(d, xin[UB + c * D:UB + (c + 1) * D, :]))

    @pl.when(s < last)
    def _():
        @pl.loop(0, NB)
        def _(j):
            @pl.when(late)
            def _():
                slope_part(j)

            chain_wait(j)

            @pl.when(s > 0)
            def _():
                chain_step(j, lambda g, c: mat(g, xin[VT + c * D:VT + (c + 1) * D, :]),
                           lambda d, c: mat(d, xin[UT + c * D:UT + (c + 1) * D, :]))

            @pl.when(s == 0)
            def _():
                chain_step(j, lambda g, c: mat(g, xin[VT + c * D:VT + (c + 1) * D, :]), None)

    @pl.when(late)
    def _():
        @pl.loop(0, NB)
        def _(j):
            hidden_part(j)

        transpose_acts()

    pltpu.make_async_copy(own, own, ldg_sem).wait()

    half_d = D // 2

    def add_weight_grads(j):
        @pl.when(j < hb)
        def _():
            for half in (0, 1):
                for m in (0, 1):
                    rows = ds(half * FF + j * D + m * half_d, half_d)
                    own[rows, :] += mat(at[m * half_d:(m + 1) * half_d, :], wbuf[ds(DP + (half * hb + j) * T, T), :])

        @pl.when(j >= hb)
        def _():
            for half in (0, 1):
                for m in (0, 1):
                    rows = ds(half * FF + j * D + m * half_d, half_d)
                    own[rows, :] += mat(wbuf[ds(HT + (half * hb + j - hb) * D + m * half_d, half_d), :], gin[...])

    @pl.when(s == 0)
    def _():
        @pl.loop(0, NU)
        def _(u):
            pltpu.make_async_copy(nb.at[ds(u * UR, UR), :], xin.at[ds(u * UR, UR), :], x_recv.at[u]).start()

    def state_loads(half):
        spare = (1 - half) * FF
        out = []
        for b in range(hb):
            cols = slice((half * hb + b) * D, (half * hb + b + 1) * D)
            up, down = b * D, FF // 2 + b * D
            out.append(pltpu.make_async_copy(mu.at[:, cols], mst.at[up:up + D, :], ldm_sem.at[0]))
            out.append(pltpu.make_async_copy(md.at[cols, :], mst.at[down:down + D, :], ldm_sem.at[0]))
            out.append(pltpu.make_async_copy(m1u.at[:, cols], slope.at[up:up + D, :], ldm_sem.at[1]))
            out.append(pltpu.make_async_copy(m1d.at[cols, :], slope.at[down:down + D, :], ldm_sem.at[1]))
            out.append(pltpu.make_async_copy(m2u.at[:, cols], rbuf.at[spare + up:spare + up + D, :], ldm_sem.at[2]))
            out.append(pltpu.make_async_copy(m2d.at[cols, :], rbuf.at[spare + down:spare + down + D, :], ldm_sem.at[2]))
        return out

    for half, where in ((0, r == 0), (1, r == R - 1)):
        @pl.when(where)
        def _():
            for load in state_loads(half):
                load.start()

    def half_rows(half, k):
        return ds(half * FF + k * CR, CR)

    def await_f32(sem, half, k):
        rows = half_rows(half, k)
        pltpu.make_async_copy(own.at[rows, :], own.at[rows, :], sem.at[half, k]).wait()

    def rs_copy(src, half, k):
        rows = half_rows(half, k)
        return pltpu.make_async_remote_copy(src.at[rows, :], rbuf.at[rows, :], rs_send.at[half], rs_recv.at[half, k],
                                            device_id={"data": r + 2 * half - 1}, device_id_type=MESH)

    def half_sent(ref, sem, half):
        rows = ds(half * FF, FF)
        pltpu.make_async_copy(ref.at[rows, :], ref.at[rows, :], sem.at[half]).wait()

    rs_near = jnp.where(low, 1, 0)
    rs_far = 1 - rs_near
    lag = jnp.where(is_end, cfg.LAG_END, cfg.LAG_MID)
    sq[...] = jnp.zeros_like(sq)

    per_block = D // CR

    @pl.loop(0, K + cfg.LAG_END)
    def _(i):
        @pl.when((i % per_block == 0) & (i < K))
        def _():
            with jax.named_scope("weight_grads"):
                add_weight_grads(i // per_block)

        @pl.when((i < K) & is_end)
        def _():
            rs_copy(own, rs_near, i).start()

        @pl.when((i < K) & is_mid)
        def _():
            await_f32(rs_recv, rs_near, i)
            rows = half_rows(rs_near, i)
            rbuf[rows, :] += own[rows, :]
            rs_copy(rbuf, rs_near, i).start()

        k = i - lag

        @pl.when((k >= 0) & (k < K) & is_mid)
        def _():
            with jax.named_scope("rs_far_wait"):
                await_f32(rs_recv, rs_far, k)
            rows = half_rows(rs_far, k)
            rbuf[rows, :] += own[rows, :]
            rs_copy(rbuf, rs_far, k).start()

        @pl.when((k >= 0) & (k < K) & is_end)
        def _():
            with jax.named_scope("rs_end_wait"):
                await_f32(rs_recv, rs_far, k)
            rows = half_rows(rs_far, k)
            mean = (own[rows, :] + rbuf[rows, :]) * (1.0 / R)
            own[rows, :] = mean
            sq[...] += jnp.sum((mean * mean).reshape(CR // 8, 8, D), axis=0)

    mine = jnp.where(r == 0, s, S + s)
    me = r * S + s

    def c_copy(dev):
        return pltpu.make_async_remote_copy(cbuf.at[mine], cbuf.at[mine], c_send, c_recv.at[mine],
                                            device_id=(dev // S, dev % S), device_id_type=MESH)

    @pl.when(is_end)
    def _():
        part = sq[:, 0:128]
        for q in range(1, D // 128):
            part = part + sq[:, q * 128:(q + 1) * 128]
        cbuf[mine] = part

        half_sent(own, rs_send, rs_near)

        @pl.loop(0, R * S)
        def _(dev):
            @pl.when(dev != me)
            def _():
                c_copy(dev).start()

    with jax.named_scope("clip_wait"):
        @pl.loop(0, 2 * S)
        def _(slot):
            @pl.when(is_mid | (slot != mine))
            def _():
                pltpu.make_async_copy(cbuf.at[slot], cbuf.at[slot], c_recv.at[slot]).wait()

    total_sq = cbuf[0]
    for slot in range(1, 2 * S):
        total_sq = total_sq + cbuf[slot]
    total_sq = jnp.sum(jnp.sum(total_sq, axis=0, keepdims=True), axis=1, keepdims=True)
    grad_norm = jnp.sqrt(jnp.broadcast_to(total_sq, (8, 128)))
    cvec[...] = jnp.minimum(1.0, mn_ref[0] / (grad_norm + NORM_EPS))
    pltpu.make_async_copy(cvec, c_out, co_sem).start()

    @pl.when(is_end)
    def _():
        for n in range(3):
            pltpu.make_async_copy(mst, mst, ldm_sem.at[n]).wait()

    ag_near = 1 - rs_near
    ag_far = rs_near

    def gb_rows(half, k):
        return ds(half * FF + k * CG, CG)

    def w_copy(half, k):
        rows = gb_rows(half, k)
        return pltpu.make_async_remote_copy(wbuf.at[rows, :], wbuf.at[rows, :], w_send.at[half], rs_recv.at[half, k],
                                            device_id={"data": r + 1 - 2 * half}, device_id_type=MESH)

    def await_w(half, k):
        rows = gb_rows(half, k)
        pltpu.make_async_copy(wbuf.at[rows, :], wbuf.at[rows, :], rs_recv.at[half, k]).wait()

    @pl.loop(0, KG + cfg.GLAG_MID)
    def _(i):
        @pl.when((i < KG) & is_end)
        def _():
            rows = gb_rows(ag_near, i)
            local = ds(i * CG, CG)
            clip = cvec[0:1, 0:1]
            new_master, _, _ = adamw_update(mst[local, :], slope[local, :], rbuf[gb_rows(rs_near, i), :], own[rows, :], clip, lr_ref[0])
            wbuf[rows, :] = new_master.astype(BF16)
            w_copy(ag_near, i).start()

        @pl.when((i < KG) & is_mid)
        def _():
            with jax.named_scope("w_near_wait"):
                await_w(ag_near, i)
            w_copy(ag_near, i).start()

        k = i - cfg.GLAG_MID

        @pl.when((k >= 0) & is_mid)
        def _():
            await_w(ag_far, k)
            w_copy(ag_far, k).start()

    def await_gb(half, k):
        rows = gb_rows(half, k)
        pltpu.make_async_copy(own.at[rows, :], own.at[rows, :], gb_recv.at[half, k]).wait()

    def gb_copy(half, k):
        rows = gb_rows(half, k)
        return pltpu.make_async_remote_copy(own.at[rows, :], own.at[rows, :], gb_send.at[half], gb_recv.at[half, k],
                                            device_id={"data": r + 1 - 2 * half}, device_id_type=MESH)

    def gb_store(half, k):
        rows = gb_rows(half, k)

        @pl.when(k < KG // 2)
        def _():
            flat = k * CG
            cols = ds((half * hb + flat // D) * D, D)
            pltpu.make_async_copy(own.at[rows, :], gbu.at[ds(flat % D, CG), cols], ou_sem).start()

        @pl.when(k >= KG // 2)
        def _():
            flat = half * (FF // 2) + (k - KG // 2) * CG
            pltpu.make_async_copy(own.at[rows, :], gbd.at[ds(flat, CG), :], od_sem).start()

    g_lag = jnp.where(is_end, cfg.GLAG_END, cfg.GLAG_MID)

    def z_step(i):
        @pl.when(i < KG)
        def _():
            @pl.when(is_mid)
            def _():
                await_gb(ag_near, i)
                gb_copy(ag_near, i).start()

            gb_store(ag_near, i)

        k = i - g_lag

        @pl.when((k >= 0) & (k < KG))
        def _():
            await_gb(ag_far, k)

            @pl.when(is_mid)
            def _():
                gb_copy(ag_far, k).start()

            gb_store(ag_far, k)

    @pl.when(is_end)
    def _():
        @pl.loop(0, KG)
        def _(k):
            gb_copy(ag_near, k).start()

        @pl.loop(0, KG)
        def _(k):
            with jax.named_scope("w_end_wait"):
                await_w(ag_far, k)

    def y_copy(u):
        return pltpu.make_async_remote_copy(ybuf.at[u % NS], xin.at[ds(u * UR, UR), :], y_send.at[u % NS], x_recv.at[u],
                                            device_id={"stage": s + 1}, device_id_type=MESH)

    def y_store(u):
        return pltpu.make_async_copy(ybuf.at[u % NS], ys.at[ds(u * UR, UR), :], y_out.at[u % NS])

    def y_drain(u):
        @pl.when(s < last)
        def _():
            y_copy(u).wait_send()

        y_store(u).wait()

    def unit(u):
        rows = ds(u * UR, UR)

        @pl.when(u >= NS)
        def _():
            with jax.named_scope("y_wait"):
                y_drain(u - NS)

        with jax.named_scope("x_wait"):
            pltpu.make_async_copy(xin.at[rows, :], xin.at[rows, :], x_recv.at[u]).wait()
        x = xin[rows, :]
        total = None
        for c in range(nblk):
            hid = gelu_tanh(mat(x, wbuf[ru(c):ru(c) + D, :])).astype(BF16)
            piece = mat(hid, wbuf[rv(c):rv(c) + D, :])
            total = piece if total is None else total + piece
        ybuf[u % NS] = (x.astype(F32) + total).astype(BF16)

        @pl.when(s < last)
        def _():
            y_copy(u).start()

        y_store(u).start()

    z_total = KG + cfg.GLAG_END
    z_pre = s - 1

    with jax.named_scope("z_pre"):
        @pl.loop(0, z_pre)
        def _(i):
            z_step(i)

    @pl.loop(0, NU)
    def _(u):
        unit(u)

        @pl.when((u % 2 == 1) & (u // 2 + z_pre >= 0))
        def _():
            with jax.named_scope("z_step"):
                z_step(u // 2 + z_pre)

    with jax.named_scope("z_tail"):
        @pl.loop(NU // 2 + z_pre, z_total)
        def _(i):
            z_step(i)

    @pl.loop(NU - NS, NU)
    def _(u):
        y_drain(u)

    @pl.when(s > 0)
    def _():
        @pl.loop(0, NB)
        def _(j):
            g_copy(j).wait_send()

    @pl.when(is_end)
    def _():
        pltpu.make_async_copy(cbuf.at[0:R * S - 1], cbuf.at[0:R * S - 1], c_send).wait()

    half_sent(wbuf, w_send, ag_near)
    half_sent(own, gb_send, ag_near)

    @pl.when(is_mid)
    def _():
        half_sent(rbuf, rs_send, rs_near)
        half_sent(rbuf, rs_send, rs_far)
        half_sent(wbuf, w_send, ag_far)
        half_sent(own, gb_send, ag_far)

    pltpu.make_async_copy(gbu, gbu, ou_sem).wait()
    pltpu.make_async_copy(gbd, gbd, od_sem).wait()
    pltpu.make_async_copy(cvec, c_out, co_sem).wait()


def mega_call(cfg, lr, mn, acts, mu, md, dy, gu, gd, m1u, m1d, m2u, m2d, nb):
    D, FF, T, M = cfg.D, cfg.FF, cfg.T, cfg.M
    any_spec = pl.BlockSpec(memory_space=pl.ANY)
    smem = pl.BlockSpec(memory_space=pltpu.SMEM)
    dma = pltpu.SemaphoreType.DMA
    return pl.pallas_call(
        functools.partial(mega, cfg),
        out_shape=(
            jax.ShapeDtypeStruct((D, FF), F32),
            jax.ShapeDtypeStruct((FF, D), F32),
            jax.ShapeDtypeStruct((8, 128), F32),
            jax.ShapeDtypeStruct((M * T, D), BF16),
        ),
        in_specs=[smem, smem] + [any_spec] * 11,
        out_specs=(any_spec,) * 4,
        scratch_shapes=[
            pltpu.VMEM((2 * FF, D), F32),
            pltpu.VMEM((2 * FF, D), F32),
            pltpu.VMEM((2 * FF, D), BF16),
            pltpu.VMEM((M * T, D), BF16),
            pltpu.VMEM((cfg.NS, cfg.UR, D), BF16),
            pltpu.VMEM((T, D), BF16),
            pltpu.VMEM((T, D), BF16),
            pltpu.VMEM((max(cfg.nblk * T, FF), D), F32),
            pltpu.VMEM((FF, D), F32),
            pltpu.VMEM((T, D), BF16),
            pltpu.VMEM((D, T), BF16),
            pltpu.VMEM((8, D), F32),
            pltpu.VMEM((cfg.R * cfg.S, 8, 128), F32),
            pltpu.VMEM((8, 128), F32),
            dma,
            dma((2 * cfg.nblk,)),
            dma,
            dma((3,)),
            dma((cfg.NB,)),
            dma((cfg.NB,)),
            dma((2, cfg.K)),
            dma((2,)),
            dma((2 * cfg.S,)),
            dma,
            dma((2,)),
            dma((2, cfg.KG)),
            dma((2,)),
            dma((cfg.NU,)),
            dma((cfg.NS,)),
            dma((cfg.NS,)),
            dma,
            dma,
            dma,
        ],
        compiler_params=pltpu.CompilerParams(
            collective_id=0, has_side_effects=True, vmem_limit_bytes=67043328),
        name="pipeline_step",
    )(lr, mn, acts, mu, md, dy, gu, gd, m1u, m1d, m2u, m2d, nb)


def finish(steps, lr_ref, clip_ref, gu, gd, mu, md, m1u, m1d, m2u, m2d, rows_in,
           new_u, new_d, new_m1u, new_m1d, new_m2u, new_m2d, rows_out,
           guv, gdv, muv, mdv, m1uv, m1dv, m2uv, m2dv, rv, in_sem, out_sem):
    reads = ((gu, guv), (mu, muv), (m1u, m1uv), (m2u, m2uv), (gd, gdv), (md, mdv), (m1d, m1dv), (m2d, m2dv), (rows_in, rv))
    writes = ((muv, new_u), (m1uv, new_m1u), (m2uv, new_m2u), (mdv, new_d), (m1dv, new_m1d), (m2dv, new_m2d), (rv, rows_out))

    def part(x, i):
        size = x.shape[0] // steps
        return pl.ds(pl.multiple_of(i * size, size), size)

    def read(n, i):
        src, dst = reads[n]
        return pltpu.make_async_copy(src.at[part(src, i), :], dst.at[part(src, i), :], in_sem.at[i])

    def write(n, i):
        src, dst = writes[n]
        return pltpu.make_async_copy(src.at[part(src, i), :], dst.at[part(src, i), :], out_sem.at[n])

    @pl.loop(0, steps)
    def _(i):
        for n in range(len(reads)):
            read(n, i).start()

    clip = clip_ref[0:1, 0:1]

    @pl.loop(0, steps)
    def _(i):
        for n in range(len(reads)):
            read(n, i).wait()
        write(6, i).start()
        for g, w, m1, m2, out in ((guv, muv, m1uv, m2uv, 0), (gdv, mdv, m1dv, m2dv, 3)):
            p = part(g, i)
            w[p, :], m1[p, :], m2[p, :] = adamw_update(w[p, :], m1[p, :], m2[p, :], g[p, :], clip, lr_ref[0])
            for n in range(out, out + 3):
                write(n, i).start()

    for n in range(len(writes)):
        pltpu.make_async_copy(writes[n][0], writes[n][1], out_sem.at[n]).wait()


def finish_call(lr, clip, gu, gd, mu, md, m1u, m1d, m2u, m2d, rows_in, steps):
    ins = (gu, gd, mu, md, m1u, m1d, m2u, m2d, rows_in)
    outs = (mu, md, m1u, m1d, m2u, m2d, rows_in)
    any_spec = pl.BlockSpec(memory_space=pl.ANY)
    return pl.pallas_call(
        functools.partial(finish, steps),
        out_shape=tuple(jax.ShapeDtypeStruct(x.shape, x.dtype) for x in outs),
        in_specs=[pl.BlockSpec(memory_space=pltpu.SMEM), pl.BlockSpec(memory_space=pltpu.VMEM)] + [any_spec] * len(ins),
        out_specs=(any_spec,) * len(outs),
        scratch_shapes=[pltpu.VMEM(x.shape, x.dtype) for x in ins]
        + [pltpu.SemaphoreType.DMA((steps,)), pltpu.SemaphoreType.DMA((len(outs),))],
        compiler_params=pltpu.CompilerParams(vmem_limit_bytes=67043328),
        name="finish",
    )(lr, clip, *ins)


def solution(mesh):
    n_stages = mesh.shape['stage']
    n_reps = mesh.shape['data']

    def local_step(master_up, master_down, mom1_up, mom1_down, mom2_up, mom2_down, grad_up, grad_down, stage_acts, loss_grad, next_batch, learn_rate, max_norm):
        n_micro, rows, width = next_batch.shape
        hidden = master_up.shape[2]
        cfg = Cfg(n_reps, n_stages, width, hidden, rows, n_micro)
        gbar_up, gbar_down, clip, outs = mega_call(
            cfg, learn_rate.reshape(1), max_norm.reshape(1), stage_acts[0], master_up[0], master_down[0], loss_grad,
            grad_up[0, 0], grad_down[0, 0], mom1_up[0], mom1_down[0], mom2_up[0], mom2_down[0],
            next_batch.reshape(n_micro * rows, width))
        new_up, new_down, new_m1_up, new_m1_down, new_m2_up, new_m2_down, outs = finish_call(
            learn_rate.reshape(1), clip, gbar_up, gbar_down, master_up[0], master_down[0], mom1_up[0], mom1_down[0],
            mom2_up[0], mom2_down[0], outs, 16)
        stage_outs = outs.reshape(1, n_micro, rows, width)
        return (new_up[None], new_down[None], new_m1_up[None], new_m1_down[None], new_m2_up[None], new_m2_down[None], stage_outs)

    w_spec = P('stage', None, None)
    g_spec = P('data', 'stage', None, None)
    in_specs = (w_spec, w_spec, w_spec, w_spec, w_spec, w_spec, g_spec, g_spec, P('stage', 'data', None), P('data', None), P(None, 'data', None), P(), P())
    out_specs = (w_spec, w_spec, w_spec, w_spec, w_spec, w_spec, P('stage', None, 'data', None))
    return jax.shard_map(local_step, mesh=mesh, in_specs=in_specs, out_specs=out_specs, check_vma=False)
```

```python
import functools

import jax
import jax.numpy as jnp
from jax import lax
from jax.experimental import pallas as pl
from jax.experimental.pallas import tpu as pltpu
from jax.sharding import PartitionSpec as P

BETA1 = 0.9
BETA2 = 0.95
ADAM_EPS = 1e-8
WEIGHT_DECAY = 0.1
NORM_EPS = 1e-6
ADAM_STEP = 8
SQRT_TWO_PI = 0.7978845608028654
GELU_CUBIC = 0.044715

MESH = pl.DeviceIdType.MESH
F32 = jnp.float32
BF16 = jnp.bfloat16


def tanh_part(pre_act):
    return jnp.tanh(SQRT_TWO_PI * (pre_act + GELU_CUBIC * pre_act * pre_act * pre_act))


def gelu_tanh(pre_act):
    return 0.5 * pre_act * (1.0 + tanh_part(pre_act))


def gelu_pair(pre_act):
    tanh_val = tanh_part(pre_act)
    act_value = 0.5 * pre_act * (1.0 + tanh_val)
    act_slope = 0.5 * (1.0 + tanh_val) + 0.5 * pre_act * (1.0 - tanh_val * tanh_val) * SQRT_TWO_PI * (1.0 + 3.0 * GELU_CUBIC * pre_act * pre_act)
    return act_value, act_slope


def mat(left, right):
    return jnp.dot(left, right, preferred_element_type=F32)


def mat_nt(left, right):
    return lax.dot_general(left, right, (((1,), (1,)), ((), ())), preferred_element_type=F32)


def adamw_update(master, first_mom, second_mom, grad_avg, clip_scale, learn_rate):
    scaled = clip_scale * grad_avg
    new_first = BETA1 * first_mom + (1.0 - BETA1) * scaled
    new_second = BETA2 * second_mom + (1.0 - BETA2) * scaled * scaled
    first_hat = new_first / (1.0 - BETA1 ** ADAM_STEP)
    second_hat = new_second / (1.0 - BETA2 ** ADAM_STEP)
    new_master = master - learn_rate * (first_hat / (jnp.sqrt(second_hat) + ADAM_EPS) + WEIGHT_DECAY * master)
    return new_master, new_first, new_second


class Cfg:
    def __init__(self, reps, stages, width, hidden, rows, micro):
        self.R, self.S, self.D, self.FF, self.T, self.M = reps, stages, width, hidden, rows, micro
        self.nblk = hidden // width
        self.hb = self.nblk // 2
        self.NB = 4
        self.BR = rows // self.NB
        self.CR = width // 16
        self.K = hidden // self.CR
        self.CG = width // 8
        self.KG = hidden // self.CG
        self.UR = rows // 4
        self.NU = micro * rows // self.UR
        self.LAG_MID = 3
        self.LAG_END = 16
        self.GLAG_MID = 2
        self.GLAG_END = 8


def mega(cfg, lr_ref, mn_ref, acts, mu, md, dy, gu, gd, m1u, m1d, m2u, m2d, nb,
         own, cvec, ys,
         rbuf, wbuf, xin, gin, gout, slope, mst, av, at, sq, cbuf,
         ld_sem, ldw_sem, ldg_sem, ldm_sem, g_recv, g_send, rs_recv, rs_send, c_recv, c_send, w_send,
         gb_recv, gb_send, x_recv, y_send):
    R, S, D, FF, T, M = cfg.R, cfg.S, cfg.D, cfg.FF, cfg.T, cfg.M
    CG, KG = cfg.CG, cfg.KG
    nblk, hb, NB, BR, CR, K, UR, NU = cfg.nblk, cfg.hb, cfg.NB, cfg.BR, cfg.CR, cfg.K, cfg.UR, cfg.NU
    r = lax.axis_index("data")
    s = lax.axis_index("stage")
    last = S - 1
    is_end = (r == 0) | (r == R - 1)
    is_mid = jnp.logical_not(is_end)
    low = r < R // 2

    UB, VB, UT, VT = 0, FF, 2 * FF, 3 * FF
    HT, DP = 0, FF

    def ru(c):
        return (c // hb) * FF + (c % hb) * D

    def rv(c):
        return ru(c) + FF // 2

    def ds(start, size):
        return pl.ds(pl.multiple_of(start, size), size)

    barrier = pltpu.get_barrier_semaphore()

    @pl.loop(0, R * S)
    def _(dev):
        pl.semaphore_signal(barrier, inc=1, device_id=(dev // S, dev % S), device_id_type=MESH)

    act_load = pltpu.make_async_copy(acts, av, ld_sem)
    act_load.start()
    w_loads = []
    for c in range(nblk):
        w_loads.append(pltpu.make_async_copy(mu.at[:, c * D:(c + 1) * D], own.at[ru(c):ru(c) + D, :], ldw_sem.at[c]))
    for c in range(nblk):
        w_loads.append(pltpu.make_async_copy(md.at[c * D:(c + 1) * D, :], own.at[rv(c):rv(c) + D, :], ldw_sem.at[nblk + c]))
    for load in w_loads:
        load.start()

    @pl.when(s == last)
    def _():
        for j in range(NB):
            pltpu.make_async_copy(dy.at[j * BR:(j + 1) * BR, :], gin.at[j * BR:(j + 1) * BR, :], g_recv.at[j]).start()

    g_loads = []
    for c in range(nblk):
        g_loads.append(pltpu.make_async_copy(gu.at[:, c * D:(c + 1) * D], own.at[ru(c):ru(c) + D, :], ldg_sem))
        g_loads.append(pltpu.make_async_copy(gd.at[c * D:(c + 1) * D, :], own.at[rv(c):rv(c) + D, :], ldg_sem))

    act_load.wait()
    for c in range(nblk):
        w_loads[c].wait()
        xin[UB + c * D:UB + (c + 1) * D, :] = own[ru(c):ru(c) + D, :].astype(BF16)

    for c in range(nblk):
        w_loads[nblk + c].wait()
        xin[VB + c * D:VB + (c + 1) * D, :] = own[rv(c):rv(c) + D, :].astype(BF16)
    for load in g_loads:
        load.start()

    late = s >= S // 2

    def slope_part(j):
        for c in range(nblk):
            pre = mat(av[ds(j * BR, BR), :], xin[UB + c * D:UB + (c + 1) * D, :])
            _, act_slope = gelu_pair(pre)
            slope[ds(c * T + j * BR, BR), :] = act_slope

    def hidden_part(j):
        @pl.loop(0, nblk)
        def _(c):
            pre = mat(av[ds(j * BR, BR), :], xin[ds(UB + c * D, D), :])
            wbuf[ds(HT + c * D, D), ds(j * BR, BR)] = gelu_tanh(pre).T.astype(BF16)

    def transpose_acts():
        at[...] = av[...].astype(F32).T.astype(BF16)

    @pl.when(s < last)
    def _():
        @pl.loop(0, nblk)
        def _(c):
            xin[ds(UT + c * D, D), :] = xin[ds(UB + c * D, D), :].T
            xin[ds(VT + c * D, D), :] = xin[ds(VB + c * D, D), :].T

    @pl.when(s < last - 1)
    def _():
        @pl.loop(0, NB)
        def _(j):
            slope_part(j)

    @pl.when(jnp.logical_not(late))
    def _():
        @pl.loop(0, NB)
        def _(j):
            hidden_part(j)

        transpose_acts()

    with jax.named_scope("barrier_wait"):
        pl.semaphore_wait(barrier, R * S)

    def g_copy(j):
        rows = ds(j * BR, BR)
        return pltpu.make_async_remote_copy(gout.at[rows, :], gin.at[rows, :], g_send.at[j], g_recv.at[j],
                                            device_id={"stage": s - 1}, device_id_type=MESH)

    def chain_step(j, down_of, up_of, beside=None):
        rows = ds(j * BR, BR)
        g = gin[rows, :]
        total = None
        for c in range(nblk):
            part = ds(c * T + j * BR, BR)
            d_pre = (down_of(g, c) * slope[part, :]).astype(BF16)
            wbuf[ds(DP + c * T + j * BR, BR), :] = d_pre
            if up_of is not None:
                piece = up_of(d_pre, c)
                total = piece if total is None else total + piece
        if up_of is not None:
            gout[rows, :] = (g.astype(F32) + total).astype(BF16)
        if beside is not None:
            beside()
        if up_of is not None:
            g_copy(j).start()

    def chain_wait(j):
        rows = ds(j * BR, BR)
        with jax.named_scope("chain_wait"):
            pltpu.make_async_copy(gin.at[rows, :], gin.at[rows, :], g_recv.at[j]).wait()

    def down_t(g, c):
        return mat(g, xin[VT + c * D:VT + (c + 1) * D, :])

    def up_t(d, c):
        return mat(d, xin[UT + c * D:UT + (c + 1) * D, :])

    @pl.when(s == last)
    def _():
        slope_part(0)
        for j in range(NB):
            chain_wait(j)
        for j in range(NB):
            chain_step(j, lambda g, c: mat_nt(g, xin[VB + c * D:VB + (c + 1) * D, :]),
                       lambda d, c: mat_nt(d, xin[UB + c * D:UB + (c + 1) * D, :]),
                       functools.partial(slope_part, j + 1) if j + 1 < NB else None)

    @pl.when(s == last - 1)
    def _():
        slope_part(0)

        @pl.loop(0, NB)
        def _(j):
            chain_wait(j)
            chain_step(j, down_t, up_t, lambda: slope_part(jnp.minimum(j + 1, NB - 1)))

    @pl.when((s > 0) & (s < last - 1))
    def _():
        @pl.loop(0, NB)
        def _(j):
            chain_wait(j)
            chain_step(j, down_t, up_t)

    @pl.when(s == 0)
    def _():
        @pl.loop(0, NB)
        def _(j):
            chain_wait(j)
            chain_step(j, down_t, None)

    @pl.when(late)
    def _():
        @pl.loop(0, NB)
        def _(j):
            hidden_part(j)

        transpose_acts()

    pltpu.make_async_copy(own, own, ldg_sem).wait()

    half_d = D // 2

    def add_weight_grads(j):
        @pl.when(j < hb)
        def _():
            for half in (0, 1):
                for m in (0, 1):
                    rows = ds(half * FF + j * D + m * half_d, half_d)
                    own[rows, :] += mat(at[m * half_d:(m + 1) * half_d, :], wbuf[ds(DP + (half * hb + j) * T, T), :])

        @pl.when(j >= hb)
        def _():
            for half in (0, 1):
                for m in (0, 1):
                    rows = ds(half * FF + j * D + m * half_d, half_d)
                    own[rows, :] += mat(wbuf[ds(HT + (half * hb + j - hb) * D + m * half_d, half_d), :], gin[...])

    @pl.when(s == 0)
    def _():
        @pl.loop(0, NU)
        def _(u):
            pltpu.make_async_copy(nb.at[ds(u * UR, UR), :], xin.at[ds(u * UR, UR), :], x_recv.at[u]).start()

    def state_loads(half):
        spare = (1 - half) * FF
        out = []
        for b in range(hb):
            cols = slice((half * hb + b) * D, (half * hb + b + 1) * D)
            up, down = b * D, FF // 2 + b * D
            out.append(pltpu.make_async_copy(mu.at[:, cols], mst.at[up:up + D, :], ldm_sem.at[0]))
            out.append(pltpu.make_async_copy(md.at[cols, :], mst.at[down:down + D, :], ldm_sem.at[0]))
            out.append(pltpu.make_async_copy(m1u.at[:, cols], slope.at[up:up + D, :], ldm_sem.at[1]))
            out.append(pltpu.make_async_copy(m1d.at[cols, :], slope.at[down:down + D, :], ldm_sem.at[1]))
            out.append(pltpu.make_async_copy(m2u.at[:, cols], rbuf.at[spare + up:spare + up + D, :], ldm_sem.at[2]))
            out.append(pltpu.make_async_copy(m2d.at[cols, :], rbuf.at[spare + down:spare + down + D, :], ldm_sem.at[2]))
        return out

    for half, where in ((0, r == 0), (1, r == R - 1)):
        @pl.when(where)
        def _():
            for load in state_loads(half):
                load.start()

    def half_rows(half, k):
        return ds(half * FF + k * CR, CR)

    def await_f32(sem, half, k):
        rows = half_rows(half, k)
        pltpu.make_async_copy(own.at[rows, :], own.at[rows, :], sem.at[half, k]).wait()

    def rs_copy(src, half, k):
        rows = half_rows(half, k)
        return pltpu.make_async_remote_copy(src.at[rows, :], rbuf.at[rows, :], rs_send.at[half], rs_recv.at[half, k],
                                            device_id={"data": r + 2 * half - 1}, device_id_type=MESH)

    def half_sent(ref, sem, half):
        rows = ds(half * FF, FF)
        pltpu.make_async_copy(ref.at[rows, :], ref.at[rows, :], sem.at[half]).wait()

    rs_near = jnp.where(low, 1, 0)
    rs_far = 1 - rs_near
    lag = jnp.where(is_end, cfg.LAG_END, cfg.LAG_MID)
    sq[...] = jnp.zeros_like(sq)

    per_block = D // CR

    @pl.loop(0, K + cfg.LAG_END)
    def _(i):
        @pl.when((i % per_block == 0) & (i < K))
        def _():
            with jax.named_scope("weight_grads"):
                add_weight_grads(i // per_block)

        @pl.when((i < K) & is_end)
        def _():
            rs_copy(own, rs_near, i).start()

        @pl.when((i < K) & is_mid)
        def _():
            await_f32(rs_recv, rs_near, i)
            rows = half_rows(rs_near, i)
            rbuf[rows, :] += own[rows, :]
            rs_copy(rbuf, rs_near, i).start()

        k = i - lag

        @pl.when((k >= 0) & (k < K) & is_mid)
        def _():
            with jax.named_scope("rs_far_wait"):
                await_f32(rs_recv, rs_far, k)
            rows = half_rows(rs_far, k)
            rbuf[rows, :] += own[rows, :]
            rs_copy(rbuf, rs_far, k).start()

        @pl.when((k >= 0) & (k < K) & is_end)
        def _():
            with jax.named_scope("rs_end_wait"):
                await_f32(rs_recv, rs_far, k)
            rows = half_rows(rs_far, k)
            mean = (own[rows, :] + rbuf[rows, :]) * (1.0 / R)
            own[rows, :] = mean
            sq[...] += jnp.sum((mean * mean).reshape(CR // 8, 8, D), axis=0)

    mine = jnp.where(r == 0, s, S + s)
    me = r * S + s

    def c_copy(dev):
        return pltpu.make_async_remote_copy(cbuf.at[mine], cbuf.at[mine], c_send, c_recv.at[mine],
                                            device_id=(dev // S, dev % S), device_id_type=MESH)

    @pl.when(is_end)
    def _():
        part = sq[:, 0:128]
        for q in range(1, D // 128):
            part = part + sq[:, q * 128:(q + 1) * 128]
        cbuf[mine] = part

        half_sent(own, rs_send, rs_near)

        @pl.loop(0, R * S)
        def _(dev):
            @pl.when(dev != me)
            def _():
                c_copy(dev).start()

    with jax.named_scope("clip_wait"):
        @pl.loop(0, 2 * S)
        def _(slot):
            @pl.when(is_mid | (slot != mine))
            def _():
                pltpu.make_async_copy(cbuf.at[slot], cbuf.at[slot], c_recv.at[slot]).wait()

    total_sq = cbuf[0]
    for slot in range(1, 2 * S):
        total_sq = total_sq + cbuf[slot]
    total_sq = jnp.sum(jnp.sum(total_sq, axis=0, keepdims=True), axis=1, keepdims=True)
    grad_norm = jnp.sqrt(jnp.broadcast_to(total_sq, (8, 128)))
    cvec[...] = jnp.minimum(1.0, mn_ref[0] / (grad_norm + NORM_EPS))

    @pl.when(is_end)
    def _():
        for n in range(3):
            pltpu.make_async_copy(mst, mst, ldm_sem.at[n]).wait()

    ag_near = 1 - rs_near
    ag_far = rs_near

    def gb_rows(half, k):
        return ds(half * FF + k * CG, CG)

    def w_copy(half, k):
        rows = gb_rows(half, k)
        return pltpu.make_async_remote_copy(wbuf.at[rows, :], wbuf.at[rows, :], w_send.at[half], rs_recv.at[half, k],
                                            device_id={"data": r + 1 - 2 * half}, device_id_type=MESH)

    def await_w(half, k):
        rows = gb_rows(half, k)
        pltpu.make_async_copy(wbuf.at[rows, :], wbuf.at[rows, :], rs_recv.at[half, k]).wait()

    @pl.loop(0, KG + cfg.GLAG_MID)
    def _(i):
        @pl.when((i < KG) & is_end)
        def _():
            rows = gb_rows(ag_near, i)
            local = ds(i * CG, CG)
            clip = cvec[0:1, 0:1]
            new_master, _, _ = adamw_update(mst[local, :], slope[local, :], rbuf[gb_rows(rs_near, i), :], own[rows, :], clip, lr_ref[0])
            wbuf[rows, :] = new_master.astype(BF16)
            w_copy(ag_near, i).start()

        @pl.when((i < KG) & is_mid)
        def _():
            with jax.named_scope("w_near_wait"):
                await_w(ag_near, i)
            w_copy(ag_near, i).start()

        k = i - cfg.GLAG_MID

        @pl.when((k >= 0) & is_mid)
        def _():
            await_w(ag_far, k)
            w_copy(ag_far, k).start()

    def await_gb(half, k):
        rows = gb_rows(half, k)
        pltpu.make_async_copy(own.at[rows, :], own.at[rows, :], gb_recv.at[half, k]).wait()

    def gb_copy(half, k):
        rows = gb_rows(half, k)
        return pltpu.make_async_remote_copy(own.at[rows, :], own.at[rows, :], gb_send.at[half], gb_recv.at[half, k],
                                            device_id={"data": r + 1 - 2 * half}, device_id_type=MESH)

    g_lag = jnp.where(is_end, cfg.GLAG_END, cfg.GLAG_MID)

    def z_step(i):
        @pl.when(i < KG)
        def _():
            @pl.when(is_mid)
            def _():
                await_gb(ag_near, i)
                gb_copy(ag_near, i).start()

        k = i - g_lag

        @pl.when((k >= 0) & (k < KG))
        def _():
            await_gb(ag_far, k)

            @pl.when(is_mid)
            def _():
                gb_copy(ag_far, k).start()

    @pl.when(is_end)
    def _():
        @pl.loop(0, KG)
        def _(k):
            gb_copy(ag_near, k).start()

        @pl.loop(0, KG)
        def _(k):
            with jax.named_scope("w_end_wait"):
                await_w(ag_far, k)

    def y_copy(u):
        rows = ds(u * UR, UR)
        return pltpu.make_async_remote_copy(ys.at[rows, :], xin.at[rows, :], y_send, x_recv.at[u],
                                            device_id={"stage": s + 1}, device_id_type=MESH)

    def unit(u):
        rows = ds(u * UR, UR)

        with jax.named_scope("x_wait"):
            pltpu.make_async_copy(xin.at[rows, :], xin.at[rows, :], x_recv.at[u]).wait()
        x = xin[rows, :]
        total = None
        for c in range(nblk):
            hid = gelu_tanh(mat(x, wbuf[ru(c):ru(c) + D, :])).astype(BF16)
            piece = mat(hid, wbuf[rv(c):rv(c) + D, :])
            total = piece if total is None else total + piece
        ys[rows, :] = (x.astype(F32) + total).astype(BF16)

        @pl.when(s < last)
        def _():
            y_copy(u).start()

    z_total = KG + cfg.GLAG_END
    z_pre = s - 1

    with jax.named_scope("z_pre"):
        @pl.loop(0, z_pre)
        def _(i):
            z_step(i)

    @pl.loop(0, NU)
    def _(u):
        unit(u)

        @pl.when((u % 2 == 1) & (u // 2 + z_pre >= 0))
        def _():
            with jax.named_scope("z_step"):
                z_step(u // 2 + z_pre)

    with jax.named_scope("z_tail"):
        @pl.loop(NU // 2 + z_pre, z_total)
        def _(i):
            z_step(i)

    @pl.when(s < last)
    def _():
        pltpu.make_async_copy(ys, ys, y_send).wait()

    @pl.when(s > 0)
    def _():
        @pl.loop(0, NB)
        def _(j):
            g_copy(j).wait_send()

    @pl.when(is_end)
    def _():
        pltpu.make_async_copy(cbuf.at[0:R * S - 1], cbuf.at[0:R * S - 1], c_send).wait()

    half_sent(wbuf, w_send, ag_near)
    half_sent(own, gb_send, ag_near)

    @pl.when(is_mid)
    def _():
        half_sent(rbuf, rs_send, rs_near)
        half_sent(rbuf, rs_send, rs_far)
        half_sent(wbuf, w_send, ag_far)
        half_sent(own, gb_send, ag_far)


def mega_call(cfg, lr, mn, acts, mu, md, dy, gu, gd, m1u, m1d, m2u, m2d, nb):
    D, FF, T, M = cfg.D, cfg.FF, cfg.T, cfg.M
    any_spec = pl.BlockSpec(memory_space=pl.ANY)
    smem = pl.BlockSpec(memory_space=pltpu.SMEM)
    vmem_spec = pl.BlockSpec(memory_space=pltpu.VMEM)
    dma = pltpu.SemaphoreType.DMA
    return pl.pallas_call(
        functools.partial(mega, cfg),
        out_shape=(
            pltpu.VMEM((2 * FF, D), F32),
            pltpu.VMEM((8, 128), F32),
            pltpu.VMEM((M * T, D), BF16),
        ),
        in_specs=[smem, smem] + [pl.BlockSpec(memory_space=pltpu.HBM)] * 11,
        out_specs=(vmem_spec,) * 3,
        scratch_shapes=[
            pltpu.VMEM((2 * FF, D), F32),
            pltpu.VMEM((2 * FF, D), BF16),
            pltpu.VMEM((M * T, D), BF16),
            pltpu.VMEM((T, D), BF16),
            pltpu.VMEM((T, D), BF16),
            pltpu.VMEM((max(cfg.nblk * T, FF), D), F32),
            pltpu.VMEM((FF, D), F32),
            pltpu.VMEM((T, D), BF16),
            pltpu.VMEM((D, T), BF16),
            pltpu.VMEM((8, D), F32),
            pltpu.VMEM((cfg.R * cfg.S, 8, 128), F32),
            dma,
            dma((2 * cfg.nblk,)),
            dma,
            dma((3,)),
            dma((cfg.NB,)),
            dma((cfg.NB,)),
            dma((2, cfg.K)),
            dma((2,)),
            dma((2 * cfg.S,)),
            dma,
            dma((2,)),
            dma((2, cfg.KG)),
            dma((2,)),
            dma((cfg.NU,)),
            dma,
        ],
        compiler_params=pltpu.CompilerParams(
            collective_id=0, has_side_effects=True, vmem_limit_bytes=32 * 1024 * 1024),
        cost_estimate=pl.CostEstimate(flops=200_000_000_000, bytes_accessed=100_000_000, transcendentals=0),
        name="pipeline_step",
    )(lr, mn, *[pltpu.with_memory_space_constraint(x, pltpu.HBM) for x in (acts, mu, md, dy, gu, gd, m1u, m1d, m2u, m2d, nb)])


def finish(steps, lr_ref, clip_ref, grads, rows_in, h0, h1, h2, s0, s1, s2,
           new_u, new_d, new_m1u, new_m1d, new_m2u, new_m2d, rows_out,
           v0, v1, v2, ou, od, om1u, om1d, om2u, om2d, in_sem, out_sem, row_sem):
    mu, md, m1u, m1d, m2u, m2d = h0, v0, h1, v1, h2, v2
    outs = ((ou, new_u), (om1u, new_m1u), (om2u, new_m2u), (od, new_d), (om1d, new_m1d), (om2d, new_m2d))
    slots = ou.shape[0]
    width, hidden = mu.shape
    blocks = hidden // width

    def part(x, i):
        size = x.shape[0] // steps
        return pl.ds(pl.multiple_of(i * size, size), size)

    def row_write(i):
        return pltpu.make_async_copy(rows_in.at[part(rows_in, i), :], rows_out.at[part(rows_in, i), :], row_sem)

    def write(n, i):
        src, dst = outs[n]
        return pltpu.make_async_copy(src.at[i % slots], dst.at[part(dst, i), :], out_sem.at[n // 3, i % slots])

    def state_reads(i):
        return [pltpu.make_async_copy(src.at[part(src, i), :], dst.at[part(src, i), :], in_sem.at[i])
                for src, dst in ((s0, v0), (s1, v1), (s2, v2))]

    @pl.loop(0, steps)
    def _(i):
        for copy in state_reads(i):
            copy.start()

    clip = clip_ref[0:1, 0:1]

    @pl.loop(0, steps)
    def _(i):
        @pl.when(i >= slots)
        def _():
            for n in range(3):
                write(n, i - slots).wait()

        p = part(mu, i)
        for c in range(blocks):
            cols = slice(c * width, (c + 1) * width)
            first = (c // (blocks // 2)) * hidden + (c % (blocks // 2)) * width
            g = grads[pl.ds(pl.multiple_of(first + i * (width // steps), width // steps), width // steps), :]
            new = adamw_update(mu[p, cols], m1u[p, cols], m2u[p, cols], g, clip, lr_ref[0])
            for (dst, _), val in zip(outs[0:3], new):
                dst[i % slots, :, cols] = val
        for n in range(3):
            write(n, i).start()
        row_write(i).start()

    @pl.loop(0, steps)
    def _(i):
        @pl.when(i >= slots)
        def _():
            for n in range(3, 6):
                write(n, i - slots).wait()

        for copy in state_reads(i):
            copy.wait()
        p = part(md, i)
        size = hidden // steps
        low = i * size
        first = jnp.where(low < hidden // 2, hidden // 2 + low, hidden + low)
        g = grads[pl.ds(pl.multiple_of(first, size), size), :]
        for (dst, _), val in zip(outs[3:6], adamw_update(md[p, :], m1d[p, :], m2d[p, :], g, clip, lr_ref[0])):
            dst[i % slots] = val
        for n in range(3, 6):
            write(n, i).start()

    @pl.loop(steps - slots, steps)
    def _(i):
        for n in range(len(outs)):
            write(n, i).wait()

    pltpu.make_async_copy(rows_in, rows_out, row_sem).wait()


def finish_call(lr, clip, grads, mu, md, m1u, m1d, m2u, m2d, rows_in, steps):
    states = (mu, md, m1u, m1d, m2u, m2d)
    held, streamed = (mu, m1u, m2u), (md, m1d, m2d)
    outs = states + (rows_in,)
    any_spec = pl.BlockSpec(memory_space=pl.ANY)
    vmem_spec = pl.BlockSpec(memory_space=pltpu.VMEM)
    slots = 3

    def ring(x, n):
        return pltpu.VMEM((n, x.shape[0] // steps, x.shape[1]), x.dtype)

    dma = pltpu.SemaphoreType.DMA
    return pl.pallas_call(
        functools.partial(finish, steps),
        out_shape=tuple(jax.ShapeDtypeStruct(x.shape, x.dtype) for x in outs),
        in_specs=[pl.BlockSpec(memory_space=pltpu.SMEM), vmem_spec, vmem_spec, vmem_spec] + [vmem_spec] * 3 + [pl.BlockSpec(memory_space=pltpu.HBM)] * 3,
        out_specs=(any_spec,) * len(outs),
        scratch_shapes=[pltpu.VMEM(x.shape, F32) for x in streamed]
        + [ring(x, slots) for x in states] + [dma((steps,)), dma((2, slots)), dma],
        compiler_params=pltpu.CompilerParams(vmem_limit_bytes=20 * 1024 * 1024),
        cost_estimate=pl.CostEstimate(flops=100_000_000, bytes_accessed=75_000_000, transcendentals=0),
        name="finish",
    )(lr, clip, grads, rows_in, *[pltpu.with_memory_space_constraint(x, pltpu.VMEM) for x in held],
      *[pltpu.with_memory_space_constraint(x, pltpu.HBM) for x in streamed])


def solution(mesh):
    n_stages = mesh.shape['stage']
    n_reps = mesh.shape['data']

    def local_step(master_up, master_down, mom1_up, mom1_down, mom2_up, mom2_down, grad_up, grad_down, stage_acts, loss_grad, next_batch, learn_rate, max_norm):
        n_micro, rows, width = next_batch.shape
        hidden = master_up.shape[2]
        cfg = Cfg(n_reps, n_stages, width, hidden, rows, n_micro)
        grads, clip, outs = mega_call(
            cfg, learn_rate.reshape(1), max_norm.reshape(1), stage_acts[0], master_up[0], master_down[0], loss_grad,
            grad_up[0, 0], grad_down[0, 0], mom1_up[0], mom1_down[0], mom2_up[0], mom2_down[0],
            next_batch.reshape(n_micro * rows, width))
        new_up, new_down, new_m1_up, new_m1_down, new_m2_up, new_m2_down, outs = finish_call(
            learn_rate.reshape(1), clip, grads, master_up[0], master_down[0], mom1_up[0], mom1_down[0],
            mom2_up[0], mom2_down[0], outs, 16)
        stage_outs = outs.reshape(1, n_micro, rows, width)
        return (new_up[None], new_down[None], new_m1_up[None], new_m1_down[None], new_m2_up[None], new_m2_down[None], stage_outs)

    w_spec = P('stage', None, None)
    g_spec = P('data', 'stage', None, None)
    in_specs = (w_spec, w_spec, w_spec, w_spec, w_spec, w_spec, g_spec, g_spec, P('stage', 'data', None), P('data', None), P(None, 'data', None), P(), P())
    out_specs = (w_spec, w_spec, w_spec, w_spec, w_spec, w_spec, P('stage', None, 'data', None))
    return jax.shard_map(local_step, mesh=mesh, in_specs=in_specs, out_specs=out_specs, check_vma=False)
```

```python
import functools

import jax
import jax.numpy as jnp
from jax import lax
from jax.experimental import pallas as pl
from jax.experimental.pallas import tpu as pltpu
from jax.sharding import PartitionSpec as P

BETA1 = 0.9
BETA2 = 0.95
ADAM_EPS = 1e-8
WEIGHT_DECAY = 0.1
NORM_EPS = 1e-6
ADAM_STEP = 8
SQRT_TWO_PI = 0.7978845608028654
GELU_CUBIC = 0.044715

MESH = pl.DeviceIdType.MESH
F32 = jnp.float32
BF16 = jnp.bfloat16


def tanh_part(pre_act):
    return jnp.tanh(SQRT_TWO_PI * (pre_act + GELU_CUBIC * pre_act * pre_act * pre_act))


def gelu_tanh(pre_act):
    return 0.5 * pre_act * (1.0 + tanh_part(pre_act))


def gelu_pair(pre_act):
    tanh_val = tanh_part(pre_act)
    act_value = 0.5 * pre_act * (1.0 + tanh_val)
    act_slope = 0.5 * (1.0 + tanh_val) + 0.5 * pre_act * (1.0 - tanh_val * tanh_val) * SQRT_TWO_PI * (1.0 + 3.0 * GELU_CUBIC * pre_act * pre_act)
    return act_value, act_slope


def mat(left, right):
    return jnp.dot(left, right, preferred_element_type=F32)


def mat_nt(left, right):
    return lax.dot_general(left, right, (((1,), (1,)), ((), ())), preferred_element_type=F32)


def adamw_update(master, first_mom, second_mom, grad_avg, clip_scale, learn_rate):
    scaled = clip_scale * grad_avg
    new_first = BETA1 * first_mom + (1.0 - BETA1) * scaled
    new_second = BETA2 * second_mom + (1.0 - BETA2) * scaled * scaled
    first_hat = new_first * (1.0 / (1.0 - BETA1 ** ADAM_STEP))
    second_hat = new_second * (1.0 / (1.0 - BETA2 ** ADAM_STEP))
    new_master = master - learn_rate * (first_hat / (jnp.sqrt(second_hat) + ADAM_EPS) + WEIGHT_DECAY * master)
    return new_master, new_first, new_second


class Cfg:
    def __init__(self, reps, stages, width, hidden, rows, micro):
        self.R, self.S, self.D, self.FF, self.T, self.M = reps, stages, width, hidden, rows, micro
        self.nblk = hidden // width
        self.hb = self.nblk // 2
        self.NB = 4
        self.BR = rows // self.NB
        self.CR = width // 16
        self.K = hidden // self.CR
        self.CG = width // 8
        self.KG = hidden // self.CG
        self.UR = rows // 4
        self.NU = micro * rows // self.UR
        self.LAG_MID = 3
        self.LAG_END = 16
        self.GLAG_MID = 2
        self.GLAG_END = 8


def mega(cfg, lr_ref, mn_ref, acts, mu, md, dy, gu, gd, m1u, m1d, m2u, m2d, nb,
         own, cvec, ys,
         rbuf, wbuf, xin, gin, gout, slope, mst, av, at, sq, cbuf,
         ld_sem, ldw_sem, ldg_sem, ldm_sem, g_recv, g_send, rs_recv, rs_send, c_recv, c_send, w_send,
         gb_recv, gb_send, x_recv, y_send):
    R, S, D, FF, T, M = cfg.R, cfg.S, cfg.D, cfg.FF, cfg.T, cfg.M
    CG, KG = cfg.CG, cfg.KG
    nblk, hb, NB, BR, CR, K, UR, NU = cfg.nblk, cfg.hb, cfg.NB, cfg.BR, cfg.CR, cfg.K, cfg.UR, cfg.NU
    r = lax.axis_index("data")
    s = lax.axis_index("stage")
    last = S - 1
    is_end = (r == 0) | (r == R - 1)
    is_mid = jnp.logical_not(is_end)
    low = r < R // 2

    UB, VB, UT, VT = 0, FF, 2 * FF, 3 * FF
    HT, DP = 0, FF

    def ru(c):
        return (c // hb) * FF + (c % hb) * D

    def rv(c):
        return ru(c) + FF // 2

    def ds(start, size):
        return pl.ds(pl.multiple_of(start, size), size)

    barrier = pltpu.get_barrier_semaphore()

    @pl.loop(0, R * S)
    def _(dev):
        pl.semaphore_signal(barrier, inc=1, device_id=(dev // S, dev % S), device_id_type=MESH)

    act_load = pltpu.make_async_copy(acts, av, ld_sem)
    act_load.start()
    w_loads = []
    for c in range(nblk):
        w_loads.append(pltpu.make_async_copy(mu.at[:, c * D:(c + 1) * D], own.at[ru(c):ru(c) + D, :], ldw_sem.at[c]))
    for c in range(nblk):
        w_loads.append(pltpu.make_async_copy(md.at[c * D:(c + 1) * D, :], own.at[rv(c):rv(c) + D, :], ldw_sem.at[nblk + c]))
    for load in w_loads:
        load.start()

    @pl.when(s == last)
    def _():
        for j in range(NB):
            pltpu.make_async_copy(dy.at[j * BR:(j + 1) * BR, :], gin.at[j * BR:(j + 1) * BR, :], g_recv.at[j]).start()

    g_loads = []
    for c in range(nblk):
        g_loads.append(pltpu.make_async_copy(gu.at[:, c * D:(c + 1) * D], own.at[ru(c):ru(c) + D, :], ldg_sem))
        g_loads.append(pltpu.make_async_copy(gd.at[c * D:(c + 1) * D, :], own.at[rv(c):rv(c) + D, :], ldg_sem))

    act_load.wait()
    for c in range(nblk):
        w_loads[c].wait()
        xin[UB + c * D:UB + (c + 1) * D, :] = own[ru(c):ru(c) + D, :].astype(BF16)

    late = s >= S // 2

    def slope_part(j):
        for c in range(nblk):
            pre = mat(av[ds(j * BR, BR), :], xin[UB + c * D:UB + (c + 1) * D, :])
            _, act_slope = gelu_pair(pre)
            slope[ds(c * T + j * BR, BR), :] = act_slope

    @pl.loop(0, NB)
    def _(j):
        slope_part(j)

    for c in range(nblk):
        w_loads[nblk + c].wait()
        xin[VB + c * D:VB + (c + 1) * D, :] = own[rv(c):rv(c) + D, :].astype(BF16)
    for load in g_loads:
        load.start()

    def hidden_part(j):
        @pl.loop(0, nblk)
        def _(c):
            pre = mat(av[ds(j * BR, BR), :], xin[ds(UB + c * D, D), :])
            wbuf[ds(HT + c * D, D), ds(j * BR, BR)] = gelu_tanh(pre).T.astype(BF16)

    def transpose_acts():
        at[...] = av[...].astype(F32).T.astype(BF16)

    @pl.when(s < last)
    def _():
        @pl.loop(0, nblk)
        def _(c):
            xin[ds(UT + c * D, D), :] = xin[ds(UB + c * D, D), :].T
            xin[ds(VT + c * D, D), :] = xin[ds(VB + c * D, D), :].T

    @pl.when(jnp.logical_not(late))
    def _():
        @pl.loop(0, NB)
        def _(j):
            hidden_part(j)

        transpose_acts()

    with jax.named_scope("barrier_wait"):
        pl.semaphore_wait(barrier, R * S)

    def g_copy(j):
        rows = ds(j * BR, BR)
        return pltpu.make_async_remote_copy(gout.at[rows, :], gin.at[rows, :], g_send.at[j], g_recv.at[j],
                                            device_id={"stage": s - 1}, device_id_type=MESH)

    def chain_step(j, down_of, up_of):
        rows = ds(j * BR, BR)
        g = gin[rows, :]
        total = None
        for c in range(nblk):
            part = ds(c * T + j * BR, BR)
            d_pre = (down_of(g, c) * slope[part, :]).astype(BF16)
            wbuf[ds(DP + c * T + j * BR, BR), :] = d_pre
            if up_of is not None:
                piece = up_of(d_pre, c)
                total = piece if total is None else total + piece
        if up_of is not None:
            gout[rows, :] = (g.astype(F32) + total).astype(BF16)
            g_copy(j).start()

    def chain_wait(j):
        rows = ds(j * BR, BR)
        with jax.named_scope("chain_wait"):
            pltpu.make_async_copy(gin.at[rows, :], gin.at[rows, :], g_recv.at[j]).wait()

    def down_t(g, c):
        return mat(g, xin[VT + c * D:VT + (c + 1) * D, :])

    def up_t(d, c):
        return mat(d, xin[UT + c * D:UT + (c + 1) * D, :])

    @pl.when(s == last)
    def _():
        @pl.loop(0, NB)
        def _(j):
            chain_wait(j)
            chain_step(j, lambda g, c: mat_nt(g, xin[VB + c * D:VB + (c + 1) * D, :]),
                       lambda d, c: mat_nt(d, xin[UB + c * D:UB + (c + 1) * D, :]))

    @pl.when((s > 0) & (s < last))
    def _():
        @pl.loop(0, NB)
        def _(j):
            chain_wait(j)
            chain_step(j, down_t, up_t)

    @pl.when(s == 0)
    def _():
        @pl.loop(0, NB)
        def _(j):
            chain_wait(j)
            chain_step(j, down_t, None)

    @pl.when(late)
    def _():
        @pl.loop(0, NB)
        def _(j):
            hidden_part(j)

        transpose_acts()

    pltpu.make_async_copy(own, own, ldg_sem).wait()

    half_d = D // 2

    def add_weight_grads(j):
        @pl.when(j < hb)
        def _():
            for half in (0, 1):
                for m in (0, 1):
                    rows = ds(half * FF + j * D + m * half_d, half_d)
                    own[rows, :] += mat(at[m * half_d:(m + 1) * half_d, :], wbuf[ds(DP + (half * hb + j) * T, T), :])

        @pl.when(j >= hb)
        def _():
            for half in (0, 1):
                for m in (0, 1):
                    rows = ds(half * FF + j * D + m * half_d, half_d)
                    own[rows, :] += mat(wbuf[ds(HT + (half * hb + j - hb) * D + m * half_d, half_d), :], gin[...])

    def state_loads(half):
        spare = (1 - half) * FF
        out = []
        for b in range(hb):
            cols = slice((half * hb + b) * D, (half * hb + b + 1) * D)
            up, down = b * D, FF // 2 + b * D
            out.append(pltpu.make_async_copy(mu.at[:, cols], mst.at[up:up + D, :], ldm_sem.at[0]))
            out.append(pltpu.make_async_copy(md.at[cols, :], mst.at[down:down + D, :], ldm_sem.at[0]))
            out.append(pltpu.make_async_copy(m1u.at[:, cols], slope.at[up:up + D, :], ldm_sem.at[1]))
            out.append(pltpu.make_async_copy(m1d.at[cols, :], slope.at[down:down + D, :], ldm_sem.at[1]))
            out.append(pltpu.make_async_copy(m2u.at[:, cols], rbuf.at[spare + up:spare + up + D, :], ldm_sem.at[2]))
            out.append(pltpu.make_async_copy(m2d.at[cols, :], rbuf.at[spare + down:spare + down + D, :], ldm_sem.at[2]))
        return out

    def half_rows(half, k):
        return ds(half * FF + k * CR, CR)

    def await_f32(sem, half, k):
        rows = half_rows(half, k)
        pltpu.make_async_copy(own.at[rows, :], own.at[rows, :], sem.at[half, k]).wait()

    def rs_copy(src, half, k):
        rows = half_rows(half, k)
        return pltpu.make_async_remote_copy(src.at[rows, :], rbuf.at[rows, :], rs_send.at[half], rs_recv.at[half, k],
                                            device_id={"data": r + 2 * half - 1}, device_id_type=MESH)

    def half_sent(ref, sem, half):
        rows = ds(half * FF, FF)
        pltpu.make_async_copy(ref.at[rows, :], ref.at[rows, :], sem.at[half]).wait()

    rs_near = jnp.where(low, 1, 0)
    rs_far = 1 - rs_near
    lag = jnp.where(is_end, cfg.LAG_END, cfg.LAG_MID)
    sq[...] = jnp.zeros_like(sq)

    per_block = D // CR

    @pl.loop(0, K + cfg.LAG_END)
    def _(i):
        @pl.when((i % per_block == 0) & (i < K))
        def _():
            with jax.named_scope("weight_grads"):
                add_weight_grads(i // per_block)

        for half, where in ((0, r == 0), (1, r == R - 1)):
            @pl.when(where & (i == K // 2))
            def _():
                for load in state_loads(half):
                    load.start()

        @pl.when((i < K) & is_end)
        def _():
            rs_copy(own, rs_near, i).start()

        @pl.when((i < K) & is_mid)
        def _():
            await_f32(rs_recv, rs_near, i)
            rows = half_rows(rs_near, i)
            rbuf[rows, :] += own[rows, :]
            rs_copy(rbuf, rs_near, i).start()

        k = i - lag

        @pl.when((k >= 0) & (k < K) & is_mid)
        def _():
            with jax.named_scope("rs_far_wait"):
                await_f32(rs_recv, rs_far, k)
            rows = half_rows(rs_far, k)
            rbuf[rows, :] += own[rows, :]
            rs_copy(rbuf, rs_far, k).start()

        @pl.when((k >= 0) & (k < K) & is_end)
        def _():
            with jax.named_scope("rs_end_wait"):
                await_f32(rs_recv, rs_far, k)
            rows = half_rows(rs_far, k)
            mean = (own[rows, :] + rbuf[rows, :]) * (1.0 / R)
            own[rows, :] = mean
            sq[...] += jnp.sum((mean * mean).reshape(CR // 8, 8, D), axis=0)

    mine = jnp.where(r == 0, s, S + s)
    me = r * S + s

    def c_copy(dev):
        return pltpu.make_async_remote_copy(cbuf.at[mine], cbuf.at[mine], c_send, c_recv.at[mine],
                                            device_id=(dev // S, dev % S), device_id_type=MESH)

    @pl.when(is_end)
    def _():
        part = sq[:, 0:128]
        for q in range(1, D // 128):
            part = part + sq[:, q * 128:(q + 1) * 128]
        cbuf[mine] = part

        half_sent(own, rs_send, rs_near)

        @pl.loop(0, R * S)
        def _(dev):
            @pl.when(dev != me)
            def _():
                c_copy(dev).start()

    @pl.when(s == 0)
    def _():
        def load(k, start, size):
            pltpu.make_async_copy(nb.at[ds(start, size), :], xin.at[ds(start, size), :], x_recv.at[k]).start()

        @pl.loop(0, NU - 1)
        def _(u):
            load(u, u * UR, UR)

        for v in range(2):
            load(NU - 1 + v, (NU - 1) * UR + v * (UR // 2), UR // 2)

    with jax.named_scope("clip_wait"):
        @pl.loop(0, 2 * S)
        def _(slot):
            @pl.when(is_mid | (slot != mine))
            def _():
                pltpu.make_async_copy(cbuf.at[slot], cbuf.at[slot], c_recv.at[slot]).wait()

    total_sq = cbuf[0]
    for slot in range(1, 2 * S):
        total_sq = total_sq + cbuf[slot]
    total_sq = jnp.sum(jnp.sum(total_sq, axis=0, keepdims=True), axis=1, keepdims=True)
    grad_norm = jnp.sqrt(jnp.broadcast_to(total_sq, (8, 128)))
    cvec[...] = jnp.minimum(1.0, mn_ref[0] / (grad_norm + NORM_EPS))

    @pl.when(is_end)
    def _():
        for n in range(3):
            pltpu.make_async_copy(mst, mst, ldm_sem.at[n]).wait()

    ag_near = 1 - rs_near
    ag_far = rs_near

    def gb_rows(half, k):
        return ds(half * FF + k * CG, CG)

    def w_copy(half, k):
        rows = gb_rows(half, k)
        return pltpu.make_async_remote_copy(wbuf.at[rows, :], wbuf.at[rows, :], w_send.at[half], rs_recv.at[half, k],
                                            device_id={"data": r + 1 - 2 * half}, device_id_type=MESH)

    def await_w(half, k):
        rows = gb_rows(half, k)
        pltpu.make_async_copy(wbuf.at[rows, :], wbuf.at[rows, :], rs_recv.at[half, k]).wait()

    @pl.loop(0, KG + cfg.GLAG_MID)
    def _(i):
        @pl.when((i < KG) & is_end)
        def _():
            rows = gb_rows(ag_near, i)
            local = ds(i * CG, CG)
            clip = cvec[0:1, 0:1]
            new_master, _, _ = adamw_update(mst[local, :], slope[local, :], rbuf[gb_rows(rs_near, i), :], own[rows, :], clip, lr_ref[0])
            wbuf[rows, :] = new_master.astype(BF16)
            w_copy(ag_near, i).start()

        @pl.when((i < KG) & is_mid)
        def _():
            with jax.named_scope("w_near_wait"):
                await_w(ag_near, i)
            w_copy(ag_near, i).start()

        k = i - cfg.GLAG_MID

        @pl.when((k >= 0) & is_mid)
        def _():
            await_w(ag_far, k)
            w_copy(ag_far, k).start()

    def await_gb(half, k):
        rows = gb_rows(half, k)
        pltpu.make_async_copy(own.at[rows, :], own.at[rows, :], gb_recv.at[half, k]).wait()

    def gb_copy(half, k):
        rows = gb_rows(half, k)
        return pltpu.make_async_remote_copy(own.at[rows, :], own.at[rows, :], gb_send.at[half], gb_recv.at[half, k],
                                            device_id={"data": r + 1 - 2 * half}, device_id_type=MESH)

    g_lag = jnp.where(is_end, cfg.GLAG_END, cfg.GLAG_MID)

    def z_step(i):
        @pl.when(i < KG)
        def _():
            @pl.when(is_mid)
            def _():
                await_gb(ag_near, i)
                gb_copy(ag_near, i).start()

        k = i - g_lag

        @pl.when((k >= 0) & (k < KG))
        def _():
            await_gb(ag_far, k)

            @pl.when(is_mid)
            def _():
                gb_copy(ag_far, k).start()

    @pl.when(is_end)
    def _():
        @pl.loop(0, KG)
        def _(k):
            gb_copy(ag_near, k).start()

        @pl.loop(0, KG)
        def _(k):
            with jax.named_scope("w_end_wait"):
                await_w(ag_far, k)

    def y_copy(k, rows):
        return pltpu.make_async_remote_copy(ys.at[rows, :], xin.at[rows, :], y_send, x_recv.at[k],
                                            device_id={"stage": s + 1}, device_id_type=MESH)

    def unit(k, start, size):
        rows = ds(start, size)

        with jax.named_scope("x_wait"):
            pltpu.make_async_copy(xin.at[rows, :], xin.at[rows, :], x_recv.at[k]).wait()
        x = xin[rows, :]
        total = None
        for c in range(nblk):
            hid = gelu_tanh(mat(x, wbuf[ru(c):ru(c) + D, :])).astype(BF16)
            piece = mat(hid, wbuf[rv(c):rv(c) + D, :])
            total = piece if total is None else total + piece
        ys[rows, :] = (x.astype(F32) + total).astype(BF16)

        @pl.when(s < last)
        def _():
            y_copy(k, rows).start()

    z_total = KG + cfg.GLAG_END
    z_pre = s - 1

    with jax.named_scope("z_pre"):
        @pl.loop(0, z_pre)
        def _(i):
            z_step(i)

    @pl.loop(0, NU - 1)
    def _(u):
        unit(u, u * UR, UR)

        @pl.when((u % 2 == 1) & (u // 2 + z_pre >= 0))
        def _():
            with jax.named_scope("z_step"):
                z_step(u // 2 + z_pre)

    @pl.loop(0, 2)
    def _(v):
        unit(NU - 1 + v, (NU - 1) * UR + v * (UR // 2), UR // 2)

    with jax.named_scope("z_tail"):
        @pl.loop((NU - 1) // 2 + z_pre, z_total)
        def _(i):
            z_step(i)

    @pl.when(s < last)
    def _():
        pltpu.make_async_copy(ys, ys, y_send).wait()

    @pl.when(s > 0)
    def _():
        @pl.loop(0, NB)
        def _(j):
            g_copy(j).wait_send()

    @pl.when(is_end)
    def _():
        pltpu.make_async_copy(cbuf.at[0:R * S - 1], cbuf.at[0:R * S - 1], c_send).wait()

    half_sent(wbuf, w_send, ag_near)
    half_sent(own, gb_send, ag_near)

    @pl.when(is_mid)
    def _():
        half_sent(rbuf, rs_send, rs_near)
        half_sent(rbuf, rs_send, rs_far)
        half_sent(wbuf, w_send, ag_far)
        half_sent(own, gb_send, ag_far)


def mega_call(cfg, lr, mn, acts, mu, md, dy, gu, gd, m1u, m1d, m2u, m2d, nb):
    D, FF, T, M = cfg.D, cfg.FF, cfg.T, cfg.M
    any_spec = pl.BlockSpec(memory_space=pl.ANY)
    smem = pl.BlockSpec(memory_space=pltpu.SMEM)
    vmem_spec = pl.BlockSpec(memory_space=pltpu.VMEM)
    dma = pltpu.SemaphoreType.DMA
    return pl.pallas_call(
        functools.partial(mega, cfg),
        out_shape=(
            pltpu.VMEM((2 * FF, D), F32),
            pltpu.VMEM((8, 128), F32),
            pltpu.VMEM((M * T, D), BF16),
        ),
        in_specs=[smem, smem] + [pl.BlockSpec(memory_space=pltpu.HBM)] * 11,
        out_specs=(vmem_spec,) * 3,
        scratch_shapes=[
            pltpu.VMEM((2 * FF, D), F32),
            pltpu.VMEM((2 * FF, D), BF16),
            pltpu.VMEM((M * T, D), BF16),
            pltpu.VMEM((T, D), BF16),
            pltpu.VMEM((T, D), BF16),
            pltpu.VMEM((max(cfg.nblk * T, FF), D), F32),
            pltpu.VMEM((FF, D), F32),
            pltpu.VMEM((T, D), BF16),
            pltpu.VMEM((D, T), BF16),
            pltpu.VMEM((8, D), F32),
            pltpu.VMEM((cfg.R * cfg.S, 8, 128), F32),
            dma,
            dma((2 * cfg.nblk,)),
            dma,
            dma((3,)),
            dma((cfg.NB,)),
            dma((cfg.NB,)),
            dma((2, cfg.K)),
            dma((2,)),
            dma((2 * cfg.S,)),
            dma,
            dma((2,)),
            dma((2, cfg.KG)),
            dma((2,)),
            dma((cfg.NU + 1,)),
            dma,
        ],
        compiler_params=pltpu.CompilerParams(
            collective_id=0, has_side_effects=True, vmem_limit_bytes=32 * 1024 * 1024),
        cost_estimate=pl.CostEstimate(flops=200_000_000_000, bytes_accessed=100_000_000, transcendentals=0),
        name="pipeline_step",
    )(lr, mn, *[pltpu.with_memory_space_constraint(x, pltpu.HBM) for x in (acts, mu, md, dy, gu, gd, m1u, m1d, m2u, m2d, nb)])


def finish(steps, lr_ref, clip_ref, grads, rows_in, h0, h1, h2, s0, s1, s2,
           new_u, new_d, new_m1u, new_m1d, new_m2u, new_m2d, rows_out,
           v0, v1, v2, ou, od, om1u, om1d, om2u, om2d, in_sem, out_sem, row_sem):
    mu, md, m1u, m1d, m2u, m2d = h0, v0, h1, v1, h2, v2
    outs = ((ou, new_u), (om1u, new_m1u), (om2u, new_m2u), (od, new_d), (om1d, new_m1d), (om2d, new_m2d))
    slots = ou.shape[0]
    width, hidden = mu.shape
    blocks = hidden // width

    def part(x, i):
        size = x.shape[0] // steps
        return pl.ds(pl.multiple_of(i * size, size), size)

    def row_write(i):
        return pltpu.make_async_copy(rows_in.at[part(rows_in, i), :], rows_out.at[part(rows_in, i), :], row_sem)

    def write(n, i):
        src, dst = outs[n]
        return pltpu.make_async_copy(src.at[i % slots], dst.at[part(dst, i), :], out_sem.at[n // 3, i % slots])

    def state_reads(i):
        return [pltpu.make_async_copy(src.at[part(src, i), :], dst.at[part(src, i), :], in_sem.at[i])
                for src, dst in ((s0, v0), (s1, v1), (s2, v2))]

    @pl.loop(0, steps)
    def _(i):
        for copy in state_reads(i):
            copy.start()

    clip = clip_ref[0:1, 0:1]

    @pl.loop(0, steps)
    def _(i):
        @pl.when(i >= slots)
        def _():
            for n in range(3):
                write(n, i - slots).wait()

        p = part(mu, i)
        for c in range(blocks):
            cols = slice(c * width, (c + 1) * width)
            first = (c // (blocks // 2)) * hidden + (c % (blocks // 2)) * width
            g = grads[pl.ds(pl.multiple_of(first + i * (width // steps), width // steps), width // steps), :]
            new = adamw_update(mu[p, cols], m1u[p, cols], m2u[p, cols], g, clip, lr_ref[0])
            for (dst, _), val in zip(outs[0:3], new):
                dst[i % slots, :, cols] = val
        for n in range(3):
            write(n, i).start()
        row_write(i).start()

    @pl.loop(0, steps)
    def _(i):
        @pl.when(i >= slots)
        def _():
            for n in range(3, 6):
                write(n, i - slots).wait()

        for copy in state_reads(i):
            copy.wait()
        p = part(md, i)
        size = hidden // steps
        low = i * size
        first = jnp.where(low < hidden // 2, hidden // 2 + low, hidden + low)
        g = grads[pl.ds(pl.multiple_of(first, size), size), :]
        for (dst, _), val in zip(outs[3:6], adamw_update(md[p, :], m1d[p, :], m2d[p, :], g, clip, lr_ref[0])):
            dst[i % slots] = val
        for n in range(3, 6):
            write(n, i).start()

    @pl.loop(steps - slots, steps)
    def _(i):
        for n in range(len(outs)):
            write(n, i).wait()

    pltpu.make_async_copy(rows_in, rows_out, row_sem).wait()


def finish_call(lr, clip, grads, mu, md, m1u, m1d, m2u, m2d, rows_in, steps):
    states = (mu, md, m1u, m1d, m2u, m2d)
    held, streamed = (mu, m1u, m2u), (md, m1d, m2d)
    outs = states + (rows_in,)
    any_spec = pl.BlockSpec(memory_space=pl.ANY)
    vmem_spec = pl.BlockSpec(memory_space=pltpu.VMEM)
    slots = 3

    def ring(x, n):
        return pltpu.VMEM((n, x.shape[0] // steps, x.shape[1]), x.dtype)

    dma = pltpu.SemaphoreType.DMA
    return pl.pallas_call(
        functools.partial(finish, steps),
        out_shape=tuple(jax.ShapeDtypeStruct(x.shape, x.dtype) for x in outs),
        in_specs=[pl.BlockSpec(memory_space=pltpu.SMEM), vmem_spec, vmem_spec, vmem_spec] + [vmem_spec] * 3 + [pl.BlockSpec(memory_space=pltpu.HBM)] * 3,
        out_specs=(any_spec,) * len(outs),
        scratch_shapes=[pltpu.VMEM(x.shape, F32) for x in streamed]
        + [ring(x, slots) for x in states] + [dma((steps,)), dma((2, slots)), dma],
        compiler_params=pltpu.CompilerParams(vmem_limit_bytes=20 * 1024 * 1024),
        cost_estimate=pl.CostEstimate(flops=100_000_000, bytes_accessed=75_000_000, transcendentals=0),
        name="finish",
    )(lr, clip, grads, rows_in, *[pltpu.with_memory_space_constraint(x, pltpu.VMEM) for x in held],
      *[pltpu.with_memory_space_constraint(x, pltpu.HBM) for x in streamed])


def solution(mesh):
    n_stages = mesh.shape['stage']
    n_reps = mesh.shape['data']

    def local_step(master_up, master_down, mom1_up, mom1_down, mom2_up, mom2_down, grad_up, grad_down, stage_acts, loss_grad, next_batch, learn_rate, max_norm):
        n_micro, rows, width = next_batch.shape
        hidden = master_up.shape[2]
        cfg = Cfg(n_reps, n_stages, width, hidden, rows, n_micro)
        grads, clip, outs = mega_call(
            cfg, learn_rate.reshape(1), max_norm.reshape(1), stage_acts[0], master_up[0], master_down[0], loss_grad,
            grad_up[0, 0], grad_down[0, 0], mom1_up[0], mom1_down[0], mom2_up[0], mom2_down[0],
            next_batch.reshape(n_micro * rows, width))
        new_up, new_down, new_m1_up, new_m1_down, new_m2_up, new_m2_down, outs = finish_call(
            learn_rate.reshape(1), clip, grads, master_up[0], master_down[0], mom1_up[0], mom1_down[0],
            mom2_up[0], mom2_down[0], outs, 16)
        stage_outs = outs.reshape(1, n_micro, rows, width)
        return (new_up[None], new_down[None], new_m1_up[None], new_m1_down[None], new_m2_up[None], new_m2_down[None], stage_outs)

    w_spec = P('stage', None, None)
    g_spec = P('data', 'stage', None, None)
    in_specs = (w_spec, w_spec, w_spec, w_spec, w_spec, w_spec, g_spec, g_spec, P('stage', 'data', None), P('data', None), P(None, 'data', None), P(), P())
    out_specs = (w_spec, w_spec, w_spec, w_spec, w_spec, w_spec, P('stage', None, 'data', None))
    return jax.shard_map(local_step, mesh=mesh, in_specs=in_specs, out_specs=out_specs, check_vma=False)
```

```python
import functools

import jax
import jax.numpy as jnp
from jax import lax
from jax.experimental import pallas as pl
from jax.experimental.pallas import tpu as pltpu
from jax.sharding import PartitionSpec as P

BETA1 = 0.9
BETA2 = 0.95
ADAM_EPS = 1e-8
WEIGHT_DECAY = 0.1
NORM_EPS = 1e-6
ADAM_STEP = 8
SQRT_TWO_PI = 0.7978845608028654
GELU_CUBIC = 0.044715

MESH = pl.DeviceIdType.MESH
F32 = jnp.float32
BF16 = jnp.bfloat16


def tanh_part(pre_act):
    return jnp.tanh(SQRT_TWO_PI * (pre_act + GELU_CUBIC * pre_act * pre_act * pre_act))


def gelu_tanh(pre_act):
    return 0.5 * pre_act * (1.0 + tanh_part(pre_act))


def gelu_pair(pre_act):
    tanh_val = tanh_part(pre_act)
    act_value = 0.5 * pre_act * (1.0 + tanh_val)
    act_slope = 0.5 * (1.0 + tanh_val) + 0.5 * pre_act * (1.0 - tanh_val * tanh_val) * SQRT_TWO_PI * (1.0 + 3.0 * GELU_CUBIC * pre_act * pre_act)
    return act_value, act_slope


def mat(left, right):
    return jnp.dot(left, right, preferred_element_type=F32)


def mat_nt(left, right):
    return lax.dot_general(left, right, (((1,), (1,)), ((), ())), preferred_element_type=F32)


def adamw_update(master, first_mom, second_mom, grad_avg, clip_scale, learn_rate):
    scaled = clip_scale * grad_avg
    new_first = BETA1 * first_mom + (1.0 - BETA1) * scaled
    new_second = BETA2 * second_mom + (1.0 - BETA2) * scaled * scaled
    first_hat = new_first * (1.0 / (1.0 - BETA1 ** ADAM_STEP))
    second_hat = new_second * (1.0 / (1.0 - BETA2 ** ADAM_STEP))
    new_master = master - learn_rate * (first_hat / (jnp.sqrt(second_hat) + ADAM_EPS) + WEIGHT_DECAY * master)
    return new_master, new_first, new_second


class Cfg:
    def __init__(self, reps, stages, width, hidden, rows, micro):
        self.R, self.S, self.D, self.FF, self.T, self.M = reps, stages, width, hidden, rows, micro
        self.nblk = hidden // width
        self.hb = self.nblk // 2
        self.NB = 4
        self.BR = rows // self.NB
        self.CR = width // 16
        self.K = hidden // self.CR
        self.CG = width // 8
        self.KG = hidden // self.CG
        self.UR = rows // 4
        self.NU = micro * rows // self.UR
        self.LAG_MID = 3
        self.LAG_END = 16
        self.GLAG_MID = 2
        self.GLAG_END = 8


def mega(cfg, lr_ref, mn_ref, acts, mu, md, dy, gu, gd, m1u, m1d, m2u, m2d, nb,
         own, cvec, ys,
         rbuf, wbuf, xin, gin, gout, slope, mst, av, at, sq, cbuf,
         ld_sem, ldw_sem, ldg_sem, ldm_sem, g_recv, g_send, rs_recv, rs_send, c_recv, c_send, w_send,
         gb_send, x_recv, y_send):
    R, S, D, FF, T, M = cfg.R, cfg.S, cfg.D, cfg.FF, cfg.T, cfg.M
    CG, KG = cfg.CG, cfg.KG
    nblk, hb, NB, BR, CR, K, UR, NU = cfg.nblk, cfg.hb, cfg.NB, cfg.BR, cfg.CR, cfg.K, cfg.UR, cfg.NU
    r = lax.axis_index("data")
    s = lax.axis_index("stage")
    last = S - 1
    is_end = (r == 0) | (r == R - 1)
    is_mid = jnp.logical_not(is_end)
    low = r < R // 2

    UB, VB, UT, VT = 0, FF, 2 * FF, 3 * FF
    HT, DP = 0, FF

    def ru(c):
        return (c // hb) * FF + (c % hb) * D

    def rv(c):
        return ru(c) + FF // 2

    def ds(start, size):
        return pl.ds(pl.multiple_of(start, size), size)

    barrier = pltpu.get_barrier_semaphore()

    @pl.loop(0, R * S)
    def _(dev):
        pl.semaphore_signal(barrier, inc=1, device_id=(dev // S, dev % S), device_id_type=MESH)

    act_load = pltpu.make_async_copy(acts, av, ld_sem)
    act_load.start()
    w_loads = []
    for c in range(nblk):
        w_loads.append(pltpu.make_async_copy(mu.at[:, c * D:(c + 1) * D], own.at[ru(c):ru(c) + D, :], ldw_sem.at[c]))
    for c in range(nblk):
        w_loads.append(pltpu.make_async_copy(md.at[c * D:(c + 1) * D, :], own.at[rv(c):rv(c) + D, :], ldw_sem.at[nblk + c]))
    for load in w_loads:
        load.start()

    @pl.when(s == last)
    def _():
        for j in range(NB):
            pltpu.make_async_copy(dy.at[j * BR:(j + 1) * BR, :], gin.at[j * BR:(j + 1) * BR, :], g_recv.at[j]).start()

    g_loads = []
    for c in range(nblk):
        g_loads.append(pltpu.make_async_copy(gu.at[:, c * D:(c + 1) * D], own.at[ru(c):ru(c) + D, :], ldg_sem))
        g_loads.append(pltpu.make_async_copy(gd.at[c * D:(c + 1) * D, :], own.at[rv(c):rv(c) + D, :], ldg_sem))

    act_load.wait()
    for c in range(nblk):
        w_loads[c].wait()
        xin[UB + c * D:UB + (c + 1) * D, :] = own[ru(c):ru(c) + D, :].astype(BF16)

    late = s >= S // 2

    def slope_part(j):
        for c in range(nblk):
            pre = mat(av[ds(j * BR, BR), :], xin[UB + c * D:UB + (c + 1) * D, :])
            _, act_slope = gelu_pair(pre)
            slope[ds(c * T + j * BR, BR), :] = act_slope

    slope_part(0)

    @pl.when(s < last - 1)
    def _():
        @pl.loop(1, NB)
        def _(j):
            slope_part(j)

    for c in range(nblk):
        w_loads[nblk + c].wait()
        xin[VB + c * D:VB + (c + 1) * D, :] = own[rv(c):rv(c) + D, :].astype(BF16)
    for load in g_loads:
        load.start()

    def hidden_part(j):
        @pl.loop(0, nblk)
        def _(c):
            pre = mat(av[ds(j * BR, BR), :], xin[ds(UB + c * D, D), :])
            wbuf[ds(HT + c * D, D), ds(j * BR, BR)] = gelu_tanh(pre).T.astype(BF16)

    def transpose_acts():
        at[...] = av[...].astype(F32).T.astype(BF16)

    @pl.when(s < last)
    def _():
        @pl.loop(0, nblk)
        def _(c):
            xin[ds(UT + c * D, D), :] = xin[ds(UB + c * D, D), :].T
            xin[ds(VT + c * D, D), :] = xin[ds(VB + c * D, D), :].T

    @pl.when(jnp.logical_not(late))
    def _():
        @pl.loop(0, NB)
        def _(j):
            hidden_part(j)

        transpose_acts()

    with jax.named_scope("barrier_wait"):
        pl.semaphore_wait(barrier, R * S)

    def g_copy(j):
        rows = ds(j * BR, BR)
        return pltpu.make_async_remote_copy(gout.at[rows, :], gin.at[rows, :], g_send.at[j], g_recv.at[j],
                                            device_id={"stage": s - 1}, device_id_type=MESH)

    def chain_step(j, down_of, up_of):
        rows = ds(j * BR, BR)
        g = gin[rows, :]
        total = None
        for c in range(nblk):
            part = ds(c * T + j * BR, BR)
            d_pre = (down_of(g, c) * slope[part, :]).astype(BF16)
            wbuf[ds(DP + c * T + j * BR, BR), :] = d_pre
            if up_of is not None:
                piece = up_of(d_pre, c)
                total = piece if total is None else total + piece
        if up_of is not None:
            gout[rows, :] = (g.astype(F32) + total).astype(BF16)
            g_copy(j).start()

    def chain_wait(j):
        rows = ds(j * BR, BR)
        with jax.named_scope("chain_wait"):
            pltpu.make_async_copy(gin.at[rows, :], gin.at[rows, :], g_recv.at[j]).wait()

    def down_t(g, c):
        return mat(g, xin[VT + c * D:VT + (c + 1) * D, :])

    def up_t(d, c):
        return mat(d, xin[UT + c * D:UT + (c + 1) * D, :])

    @pl.when(s == last)
    def _():
        @pl.loop(0, NB)
        def _(j):
            chain_wait(j)
            chain_step(j, lambda g, c: mat_nt(g, xin[VB + c * D:VB + (c + 1) * D, :]),
                       lambda d, c: mat_nt(d, xin[UB + c * D:UB + (c + 1) * D, :]))

            @pl.when(j + 1 < NB)
            def _():
                slope_part(j + 1)

    @pl.when((s > 0) & (s < last))
    def _():
        @pl.loop(0, NB)
        def _(j):
            chain_wait(j)
            chain_step(j, down_t, up_t)

            @pl.when((s == last - 1) & (j + 1 < NB))
            def _():
                slope_part(j + 1)

    @pl.when(s == 0)
    def _():
        @pl.loop(0, NB)
        def _(j):
            chain_wait(j)
            chain_step(j, down_t, None)

    @pl.when(late)
    def _():
        @pl.loop(0, NB)
        def _(j):
            hidden_part(j)

        transpose_acts()

    pltpu.make_async_copy(own, own, ldg_sem).wait()

    half_d = D // 2

    def add_weight_grads(j):
        @pl.when(j < hb)
        def _():
            for half in (0, 1):
                for m in (0, 1):
                    rows = ds(half * FF + j * D + m * half_d, half_d)
                    own[rows, :] += mat(at[m * half_d:(m + 1) * half_d, :], wbuf[ds(DP + (half * hb + j) * T, T), :])

        @pl.when(j >= hb)
        def _():
            for half in (0, 1):
                for m in (0, 1):
                    rows = ds(half * FF + j * D + m * half_d, half_d)
                    own[rows, :] += mat(wbuf[ds(HT + (half * hb + j - hb) * D + m * half_d, half_d), :], gin[...])

    def state_loads(half):
        spare = (1 - half) * FF
        out = []
        for b in range(hb):
            cols = slice((half * hb + b) * D, (half * hb + b + 1) * D)
            up, down = b * D, FF // 2 + b * D
            out.append(pltpu.make_async_copy(mu.at[:, cols], mst.at[up:up + D, :], ldm_sem.at[0]))
            out.append(pltpu.make_async_copy(md.at[cols, :], mst.at[down:down + D, :], ldm_sem.at[0]))
            out.append(pltpu.make_async_copy(m1u.at[:, cols], slope.at[up:up + D, :], ldm_sem.at[1]))
            out.append(pltpu.make_async_copy(m1d.at[cols, :], slope.at[down:down + D, :], ldm_sem.at[1]))
            out.append(pltpu.make_async_copy(m2u.at[:, cols], rbuf.at[spare + up:spare + up + D, :], ldm_sem.at[2]))
            out.append(pltpu.make_async_copy(m2d.at[cols, :], rbuf.at[spare + down:spare + down + D, :], ldm_sem.at[2]))
        return out

    def half_rows(half, k):
        return ds(half * FF + k * CR, CR)

    def await_f32(sem, half, k):
        rows = half_rows(half, k)
        pltpu.make_async_copy(own.at[rows, :], own.at[rows, :], sem.at[half, k]).wait()

    def rs_copy(src, half, k):
        rows = half_rows(half, k)
        return pltpu.make_async_remote_copy(src.at[rows, :], rbuf.at[rows, :], rs_send.at[half], rs_recv.at[half, k],
                                            device_id={"data": r + 2 * half - 1}, device_id_type=MESH)

    def half_sent(ref, sem, half):
        rows = ds(half * FF, FF)
        pltpu.make_async_copy(ref.at[rows, :], ref.at[rows, :], sem.at[half]).wait()

    rs_near = jnp.where(low, 1, 0)
    rs_far = 1 - rs_near
    lag = jnp.where(is_end, cfg.LAG_END, cfg.LAG_MID)
    sq[...] = jnp.zeros_like(sq)

    per_block = D // CR

    @pl.loop(0, K + cfg.LAG_END)
    def _(i):
        @pl.when((i % per_block == 0) & (i < K))
        def _():
            with jax.named_scope("weight_grads"):
                add_weight_grads(i // per_block)

        for half, where in ((0, r == 0), (1, r == R - 1)):
            @pl.when(where & (i == K // 2))
            def _():
                for load in state_loads(half):
                    load.start()

        @pl.when((i < K) & is_end)
        def _():
            rs_copy(own, rs_near, i).start()

        @pl.when((i < K) & is_mid)
        def _():
            await_f32(rs_recv, rs_near, i)
            rows = half_rows(rs_near, i)
            rbuf[rows, :] += own[rows, :]
            rs_copy(rbuf, rs_near, i).start()

        k = i - lag

        @pl.when((k >= 0) & (k < K) & is_mid)
        def _():
            with jax.named_scope("rs_far_wait"):
                await_f32(rs_recv, rs_far, k)
            rows = half_rows(rs_far, k)
            rbuf[rows, :] += own[rows, :]
            rs_copy(rbuf, rs_far, k).start()

        @pl.when((k >= 0) & (k < K) & is_end)
        def _():
            with jax.named_scope("rs_end_wait"):
                await_f32(rs_recv, rs_far, k)
            rows = half_rows(rs_far, k)
            mean = (own[rows, :] + rbuf[rows, :]) * (1.0 / R)
            own[rows, :] = mean
            sq[...] += jnp.sum((mean * mean).reshape(CR // 8, 8, D), axis=0)

    mine = jnp.where(r == 0, s, S + s)
    me = r * S + s

    def c_copy(dev):
        return pltpu.make_async_remote_copy(cbuf.at[mine], cbuf.at[mine], c_send, c_recv.at[mine],
                                            device_id=(dev // S, dev % S), device_id_type=MESH)

    @pl.when(is_end)
    def _():
        part = sq[:, 0:128]
        for q in range(1, D // 128):
            part = part + sq[:, q * 128:(q + 1) * 128]
        cbuf[mine] = part

        half_sent(own, rs_send, rs_near)

        @pl.loop(0, R * S)
        def _(dev):
            @pl.when(dev != me)
            def _():
                c_copy(dev).start()

    @pl.when(s == 0)
    def _():
        def load(k, start, size):
            pltpu.make_async_copy(nb.at[ds(start, size), :], xin.at[ds(start, size), :], x_recv.at[k]).start()

        @pl.loop(0, NU - 1)
        def _(u):
            load(u, u * UR, UR)

        for v in range(2):
            load(NU - 1 + v, (NU - 1) * UR + v * (UR // 2), UR // 2)

    with jax.named_scope("clip_wait"):
        @pl.loop(0, 2 * S)
        def _(slot):
            @pl.when(is_mid | (slot != mine))
            def _():
                pltpu.make_async_copy(cbuf.at[slot], cbuf.at[slot], c_recv.at[slot]).wait()

    total_sq = cbuf[0]
    for slot in range(1, 2 * S):
        total_sq = total_sq + cbuf[slot]
    total_sq = jnp.sum(jnp.sum(total_sq, axis=0, keepdims=True), axis=1, keepdims=True)
    grad_norm = jnp.sqrt(jnp.broadcast_to(total_sq, (8, 128)))
    cvec[...] = jnp.minimum(1.0, mn_ref[0] / (grad_norm + NORM_EPS))

    @pl.when(is_end)
    def _():
        for n in range(3):
            pltpu.make_async_copy(mst, mst, ldm_sem.at[n]).wait()

    ag_near = 1 - rs_near
    ag_far = rs_near

    def gb_rows(half, k):
        return ds(half * FF + k * CG, CG)

    def w_copy(half, k):
        rows = gb_rows(half, k)
        return pltpu.make_async_remote_copy(wbuf.at[rows, :], wbuf.at[rows, :], w_send.at[half], rs_recv.at[half, k],
                                            device_id={"data": r + 1 - 2 * half}, device_id_type=MESH)

    def await_w(half, k):
        rows = gb_rows(half, k)
        pltpu.make_async_copy(wbuf.at[rows, :], wbuf.at[rows, :], rs_recv.at[half, k]).wait()

    @pl.loop(0, KG + cfg.GLAG_MID)
    def _(i):
        @pl.when((i < KG) & is_end)
        def _():
            rows = gb_rows(ag_near, i)
            local = ds(i * CG, CG)
            clip = cvec[0:1, 0:1]
            new_master, _, _ = adamw_update(mst[local, :], slope[local, :], rbuf[gb_rows(rs_near, i), :], own[rows, :], clip, lr_ref[0])
            wbuf[rows, :] = new_master.astype(BF16)
            w_copy(ag_near, i).start()

        @pl.when((i < KG) & is_mid)
        def _():
            with jax.named_scope("w_near_wait"):
                await_w(ag_near, i)
            w_copy(ag_near, i).start()

        k = i - cfg.GLAG_MID

        @pl.when((k >= 0) & is_mid)
        def _():
            await_w(ag_far, k)
            w_copy(ag_far, k).start()

    def await_gb(half, k):
        rows = gb_rows(half, k)
        pltpu.make_async_copy(own.at[rows, :], own.at[rows, :], rs_recv.at[half, KG + k]).wait()

    def gb_copy(half, k):
        rows = gb_rows(half, k)
        return pltpu.make_async_remote_copy(own.at[rows, :], own.at[rows, :], gb_send.at[half], rs_recv.at[half, KG + k],
                                            device_id={"data": r + 1 - 2 * half}, device_id_type=MESH)

    g_lag = jnp.where(is_end, cfg.GLAG_END, cfg.GLAG_MID)

    def z_step(i):
        @pl.when(i < KG)
        def _():
            @pl.when(is_mid)
            def _():
                await_gb(ag_near, i)
                gb_copy(ag_near, i).start()

        k = i - g_lag

        @pl.when((k >= 0) & (k < KG))
        def _():
            await_gb(ag_far, k)

            @pl.when(is_mid)
            def _():
                gb_copy(ag_far, k).start()

    @pl.when(is_end)
    def _():
        @pl.loop(0, KG)
        def _(k):
            gb_copy(ag_near, k).start()

        @pl.loop(0, KG)
        def _(k):
            with jax.named_scope("w_end_wait"):
                await_w(ag_far, k)

    def y_copy(k, rows):
        return pltpu.make_async_remote_copy(ys.at[rows, :], xin.at[rows, :], y_send, x_recv.at[k],
                                            device_id={"stage": s + 1}, device_id_type=MESH)

    def unit(k, start, size):
        rows = ds(start, size)

        with jax.named_scope("x_wait"):
            pltpu.make_async_copy(xin.at[rows, :], xin.at[rows, :], x_recv.at[k]).wait()
        x = xin[rows, :]
        total = None
        for c in range(nblk):
            hid = gelu_tanh(mat(x, wbuf[ru(c):ru(c) + D, :])).astype(BF16)
            piece = mat(hid, wbuf[rv(c):rv(c) + D, :])
            total = piece if total is None else total + piece
        ys[rows, :] = (x.astype(F32) + total).astype(BF16)

        @pl.when(s < last)
        def _():
            y_copy(k, rows).start()

    z_total = KG + cfg.GLAG_END
    z_pre = s - 1

    with jax.named_scope("z_pre"):
        @pl.loop(0, z_pre)
        def _(i):
            z_step(i)

    @pl.loop(0, NU - 1)
    def _(u):
        unit(u, u * UR, UR)

        @pl.when((u % 2 == 1) & (u // 2 + z_pre >= 0))
        def _():
            with jax.named_scope("z_step"):
                z_step(u // 2 + z_pre)

    @pl.loop(0, 2)
    def _(v):
        unit(NU - 1 + v, (NU - 1) * UR + v * (UR // 2), UR // 2)

    with jax.named_scope("z_tail"):
        @pl.loop((NU - 1) // 2 + z_pre, z_total)
        def _(i):
            z_step(i)

    @pl.when(s < last)
    def _():
        pltpu.make_async_copy(ys, ys, y_send).wait()

    @pl.when(s > 0)
    def _():
        @pl.loop(0, NB)
        def _(j):
            g_copy(j).wait_send()

    @pl.when(is_end)
    def _():
        pltpu.make_async_copy(cbuf.at[0:R * S - 1], cbuf.at[0:R * S - 1], c_send).wait()

    half_sent(wbuf, w_send, ag_near)
    half_sent(own, gb_send, ag_near)

    @pl.when(is_mid)
    def _():
        half_sent(rbuf, rs_send, rs_near)
        half_sent(rbuf, rs_send, rs_far)
        half_sent(wbuf, w_send, ag_far)
        half_sent(own, gb_send, ag_far)


def mega_call(cfg, lr, mn, acts, mu, md, dy, gu, gd, m1u, m1d, m2u, m2d, nb):
    D, FF, T, M = cfg.D, cfg.FF, cfg.T, cfg.M
    any_spec = pl.BlockSpec(memory_space=pl.ANY)
    smem = pl.BlockSpec(memory_space=pltpu.SMEM)
    vmem_spec = pl.BlockSpec(memory_space=pltpu.VMEM)
    dma = pltpu.SemaphoreType.DMA
    return pl.pallas_call(
        functools.partial(mega, cfg),
        out_shape=(
            pltpu.VMEM((2 * FF, D), F32),
            pltpu.VMEM((8, 128), F32),
            pltpu.VMEM((M * T, D), BF16),
        ),
        in_specs=[smem, smem] + [pl.BlockSpec(memory_space=pltpu.HBM)] * 11,
        out_specs=(vmem_spec,) * 3,
        scratch_shapes=[
            pltpu.VMEM((2 * FF, D), F32),
            pltpu.VMEM((2 * FF, D), BF16),
            pltpu.VMEM((M * T, D), BF16),
            pltpu.VMEM((T, D), BF16),
            pltpu.VMEM((T, D), BF16),
            pltpu.VMEM((max(cfg.nblk * T, FF), D), F32),
            pltpu.VMEM((FF, D), F32),
            pltpu.VMEM((T, D), BF16),
            pltpu.VMEM((D, T), BF16),
            pltpu.VMEM((8, D), F32),
            pltpu.VMEM((cfg.R * cfg.S, 8, 128), F32),
            dma,
            dma((2 * cfg.nblk,)),
            dma,
            dma((3,)),
            dma((cfg.NB,)),
            dma((cfg.NB,)),
            dma((2, cfg.K)),
            dma((2,)),
            dma((2 * cfg.S,)),
            dma,
            dma((2,)),
            dma((2,)),
            dma((cfg.NU + 1,)),
            dma,
        ],
        compiler_params=pltpu.CompilerParams(
            collective_id=0, has_side_effects=True, vmem_limit_bytes=32 * 1024 * 1024),
        cost_estimate=pl.CostEstimate(flops=200_000_000_000, bytes_accessed=100_000_000, transcendentals=0),
        name="pipeline_step",
    )(lr, mn, *[pltpu.with_memory_space_constraint(x, pltpu.HBM) for x in (acts, mu, md, dy, gu, gd, m1u, m1d, m2u, m2d, nb)])


def finish(steps, lr_ref, clip_ref, grads, rows_in, h0, h1, h2, s0, s1, s2,
           new_u, new_d, new_m1u, new_m1d, new_m2u, new_m2d, rows_out,
           v0, v1, v2, ou, od, om1u, om1d, om2u, om2d, in_sem, out_sem, row_sem):
    mu, md, m1u, m1d, m2u, m2d = h0, v0, h1, v1, h2, v2
    outs = ((ou, new_u), (om1u, new_m1u), (om2u, new_m2u), (od, new_d), (om1d, new_m1d), (om2d, new_m2d))
    slots = ou.shape[0]
    width, hidden = mu.shape
    blocks = hidden // width

    def part(x, i):
        size = x.shape[0] // steps
        return pl.ds(pl.multiple_of(i * size, size), size)

    def row_write(i):
        return pltpu.make_async_copy(rows_in.at[part(rows_in, i), :], rows_out.at[part(rows_in, i), :], row_sem)

    def write(n, i):
        src, dst = outs[n]
        return pltpu.make_async_copy(src.at[i % slots], dst.at[part(dst, i), :], out_sem.at[n // 3, i % slots])

    def state_reads(i):
        return [pltpu.make_async_copy(src.at[part(src, i), :], dst.at[part(src, i), :], in_sem.at[i])
                for src, dst in ((s0, v0), (s1, v1), (s2, v2))]

    @pl.loop(0, steps)
    def _(i):
        for copy in state_reads(i):
            copy.start()

    clip = clip_ref[0:1, 0:1]

    @pl.loop(0, steps)
    def _(i):
        @pl.when(i >= slots)
        def _():
            for n in range(3):
                write(n, i - slots).wait()

        p = part(mu, i)
        for c in range(blocks):
            cols = slice(c * width, (c + 1) * width)
            first = (c // (blocks // 2)) * hidden + (c % (blocks // 2)) * width
            g = grads[pl.ds(pl.multiple_of(first + i * (width // steps), width // steps), width // steps), :]
            new = adamw_update(mu[p, cols], m1u[p, cols], m2u[p, cols], g, clip, lr_ref[0])
            for (dst, _), val in zip(outs[0:3], new):
                dst[i % slots, :, cols] = val
        for n in range(3):
            write(n, i).start()
        row_write(i).start()

    @pl.loop(0, steps)
    def _(i):
        @pl.when(i >= slots)
        def _():
            for n in range(3, 6):
                write(n, i - slots).wait()

        for copy in state_reads(i):
            copy.wait()
        p = part(md, i)
        size = hidden // steps
        low = i * size
        first = jnp.where(low < hidden // 2, hidden // 2 + low, hidden + low)
        g = grads[pl.ds(pl.multiple_of(first, size), size), :]
        for (dst, _), val in zip(outs[3:6], adamw_update(md[p, :], m1d[p, :], m2d[p, :], g, clip, lr_ref[0])):
            dst[i % slots] = val
        for n in range(3, 6):
            write(n, i).start()

    @pl.loop(steps - slots, steps)
    def _(i):
        for n in range(len(outs)):
            write(n, i).wait()

    pltpu.make_async_copy(rows_in, rows_out, row_sem).wait()


def finish_call(lr, clip, grads, mu, md, m1u, m1d, m2u, m2d, rows_in, steps):
    states = (mu, md, m1u, m1d, m2u, m2d)
    held, streamed = (mu, m1u, m2u), (md, m1d, m2d)
    outs = states + (rows_in,)
    any_spec = pl.BlockSpec(memory_space=pl.ANY)
    vmem_spec = pl.BlockSpec(memory_space=pltpu.VMEM)
    slots = 3

    def ring(x, n):
        return pltpu.VMEM((n, x.shape[0] // steps, x.shape[1]), x.dtype)

    dma = pltpu.SemaphoreType.DMA
    return pl.pallas_call(
        functools.partial(finish, steps),
        out_shape=tuple(jax.ShapeDtypeStruct(x.shape, x.dtype) for x in outs),
        in_specs=[pl.BlockSpec(memory_space=pltpu.SMEM), vmem_spec, vmem_spec, vmem_spec] + [vmem_spec] * 3 + [pl.BlockSpec(memory_space=pltpu.HBM)] * 3,
        out_specs=(any_spec,) * len(outs),
        scratch_shapes=[pltpu.VMEM(x.shape, F32) for x in streamed]
        + [ring(x, slots) for x in states] + [dma((steps,)), dma((2, slots)), dma],
        compiler_params=pltpu.CompilerParams(vmem_limit_bytes=20 * 1024 * 1024),
        cost_estimate=pl.CostEstimate(flops=100_000_000, bytes_accessed=75_000_000, transcendentals=0),
        name="finish",
    )(lr, clip, grads, rows_in, *[pltpu.with_memory_space_constraint(x, pltpu.VMEM) for x in held],
      *[pltpu.with_memory_space_constraint(x, pltpu.HBM) for x in streamed])


def solution(mesh):
    n_stages = mesh.shape['stage']
    n_reps = mesh.shape['data']

    def local_step(master_up, master_down, mom1_up, mom1_down, mom2_up, mom2_down, grad_up, grad_down, stage_acts, loss_grad, next_batch, learn_rate, max_norm):
        n_micro, rows, width = next_batch.shape
        hidden = master_up.shape[2]
        cfg = Cfg(n_reps, n_stages, width, hidden, rows, n_micro)
        grads, clip, outs = mega_call(
            cfg, learn_rate.reshape(1), max_norm.reshape(1), stage_acts[0], master_up[0], master_down[0], loss_grad,
            grad_up[0, 0], grad_down[0, 0], mom1_up[0], mom1_down[0], mom2_up[0], mom2_down[0],
            next_batch.reshape(n_micro * rows, width))
        new_up, new_down, new_m1_up, new_m1_down, new_m2_up, new_m2_down, outs = finish_call(
            learn_rate.reshape(1), clip, grads, master_up[0], master_down[0], mom1_up[0], mom1_down[0],
            mom2_up[0], mom2_down[0], outs, 16)
        stage_outs = outs.reshape(1, n_micro, rows, width)
        return (new_up[None], new_down[None], new_m1_up[None], new_m1_down[None], new_m2_up[None], new_m2_down[None], stage_outs)

    w_spec = P('stage', None, None)
    g_spec = P('data', 'stage', None, None)
    in_specs = (w_spec, w_spec, w_spec, w_spec, w_spec, w_spec, g_spec, g_spec, P('stage', 'data', None), P('data', None), P(None, 'data', None), P(), P())
    out_specs = (w_spec, w_spec, w_spec, w_spec, w_spec, w_spec, P('stage', None, 'data', None))
    return jax.shard_map(local_step, mesh=mesh, in_specs=in_specs, out_specs=out_specs, check_vma=False)
```
